128 devices in a mesh: lat: 8 (over x_lo, z), lon: 16 (over x_hi, y, core).
Axes of the slice: x: 4 (x_hi: 2, x_lo: 2; x = x_hi * 2 + x_lo), y: 4, z: 4, core: 2. Of those that a mesh axis runs over, the one named last changes fastest.
Arguments:
- latent: bfloat16 [96, 1152, 512], P('lat', 'lon'), may hold values from -1000 to 1000
- w_qkv: bfloat16 [512, 1536], replicated, may hold values from -1 to 1
- w_proj: bfloat16 [512, 512], replicated, may hold values from -0.25 to 0.25
- w_fc1: bfloat16 [512, 2048], replicated, may hold values from -0.25 to 0.25
- w_fc2: bfloat16 [2048, 512], replicated, may hold values from -0.125 to 0.125
- w_head: bfloat16 [512, 1024], replicated, may hold values from -4 to 4
- target_bins: int32 [96, 1152, 4], P('lat', 'lon'), may hold values from 0 to 255
- land_mask: int32 [96, 1152], P('lat', 'lon'), may hold values 0 or 1
Outputs:
- grad_latent: bfloat16 [96, 1152, 512], P('lat', 'lon')
- grad_qkv: float32 [512, 1536], P(('lat', 'lon'))
- grad_proj: float32 [512, 512], P(('lat', 'lon'))
- grad_fc1: float32 [512, 2048], P(('lat', 'lon'))
- grad_fc2: float32 [2048, 512], P(('lat', 'lon'))
- grad_head: float32 [512, 1024], P(('lat', 'lon'))
The draws below stay inside these ranges and needn't reach their ends.
All inputs are finite; a program needn't handle non-finite values. No bound on the sum of `land_mask` on one device may be relied on, other than what follows from the above.
Results may differ from the reference program's by a relative error of at most 0.015.
Values may be sent and summed in bfloat16 or wider, within the bound.
No kernel may reach another device: no remote copies, remote signals or barrier semaphores. Data moves between devices by JAX's collectives and lax.ppermute only.
A program may use at most 128 MiB of HBM per device.

```python
import math
import jax
import jax.numpy as jnp
from jax import lax

D = 512
HEADS = 8
FF = 2048
BINS = 256
VARS = 4
WIN_LAT = 6
WIN_LON = 12
HEAD_DIM = 64
NLAT = 96
NLON = 1152


def draw_latent(key, part):
    key_noise, key_scale, key_other = jax.random.split(jax.random.fold_in(key, 1), 3)
    noise_vals = jax.random.normal(key_noise, (NLAT, NLON, D), jnp.float32)
    token_scale = jnp.exp(jax.random.uniform(key_scale, (NLAT, NLON, 1), jnp.float32, 0.0, math.log(10.0)))
    feature_scale = jnp.exp(jax.random.uniform(key_other, (D,), jnp.float32, 0.0, math.log(10.0)))
    values_out = token_scale * feature_scale * noise_vals
    return jnp.clip(values_out, -1000.0, 1000.0).astype(jnp.bfloat16)


def draw_w_qkv(key, part):
    base_vals = jax.random.normal(jax.random.fold_in(key, 2), (D, 3 * D), jnp.float32) / math.sqrt(D)
    return jnp.clip(base_vals, -1.0, 1.0).astype(jnp.bfloat16)


def draw_w_head(key, part):
    base_vals = jax.random.normal(jax.random.fold_in(key, 4), (D, VARS * BINS), jnp.float32) * (3.0 / math.sqrt(D))
    return jnp.clip(base_vals, -4.0, 4.0).astype(jnp.bfloat16)


def plant(entries, stream_key, least, largest):
    dims = entries.shape
    index_at = [jax.random.randint(jax.random.fold_in(stream_key, axis), (), 0, dims[axis]) for axis in range(len(dims))]
    entries = entries.at[tuple(index_at)].set(least)
    longest = dims.index(max(dims))
    index_at[longest] = (index_at[longest] + 1) % dims[longest]
    return entries.at[tuple(index_at)].set(largest)


def noise(stream_key, dims, spread, most, kind=jnp.bfloat16):
    return jnp.clip(spread * jax.random.normal(stream_key, dims, jnp.float32), -most, most).astype(kind)


def setup_inputs(seed: int = 0) -> dict:
    key_of = jax.random.split(jax.random.key(seed), 9)
    latent = draw_latent(jax.random.fold_in(key_of[8], 71), 0)
    w_qkv = draw_w_qkv(jax.random.fold_in(key_of[8], 71), 0)
    w_proj = noise(key_of[2], (D, D), D ** -0.5, 0.25)
    w_fc1 = noise(key_of[3], (D, FF), D ** -0.5, 0.25)
    w_fc2 = noise(key_of[4], (FF, D), FF ** -0.5, 0.125)
    w_head = draw_w_head(jax.random.fold_in(key_of[8], 71), 0)
    target_bins = plant(jax.random.randint(key_of[6], (NLAT, NLON, VARS), 0, BINS), jax.random.fold_in(key_of[6], 1), 0, BINS - 1).astype(jnp.int32)
    land_mask = plant((jax.random.randint(key_of[7], (NLAT, NLON), 0, 4) < 3).astype(jnp.int32), jax.random.fold_in(key_of[7], 1), 0, 1)
    return dict(latent=latent, w_qkv=w_qkv, w_proj=w_proj, w_fc1=w_fc1, w_fc2=w_fc2, w_head=w_head, target_bins=target_bins, land_mask=land_mask)


eps = 1e-05
smear = 0.75
masked = -1e+30

def normalize(values_in):
    centre = lax.optimization_barrier(jnp.mean(values_in, -1, keepdims=True))
    offset = values_in - centre
    inverse = lax.rsqrt(lax.optimization_barrier(jnp.mean(offset * offset, -1, keepdims=True)) + eps)
    return (offset * inverse, inverse)

def norm_back(scaled, inverse, upstream):
    return inverse * (upstream - lax.optimization_barrier(jnp.mean(upstream, -1, keepdims=True)) - scaled * lax.optimization_barrier(jnp.mean(upstream * scaled, -1, keepdims=True)))

def gelu_parts(pre_act):
    normal_cdf = 0.5 * (1.0 + jax.scipy.special.erf(pre_act / math.sqrt(2.0)))
    density = jnp.exp(-0.5 * pre_act * pre_act) / math.sqrt(2.0 * math.pi)
    return (pre_act * normal_cdf, normal_cdf + pre_act * density)

def mixing(form, left, right):
    return jnp.einsum(form, left.astype(jnp.float32), right.astype(jnp.float32))

def to_windows(block):
    row_count, col_count, feat_count = block.shape
    shaped = block.reshape(row_count // WIN_LAT, WIN_LAT, col_count // WIN_LON, WIN_LON, feat_count)
    return shaped.transpose(0, 2, 1, 3, 4).reshape(-1, WIN_LAT * WIN_LON, feat_count)

def from_windows(packed, row_count, col_count):
    feat_count = packed.shape[-1]
    shaped = packed.reshape(row_count // WIN_LAT, col_count // WIN_LON, WIN_LAT, WIN_LON, feat_count)
    return shaped.transpose(0, 2, 1, 3, 4).reshape(row_count, col_count, feat_count)

def window_setup(qkv_all, row_labels):
    row_count, col_count, _ = qkv_all.shape
    packed = to_windows(qkv_all)
    heads_view = packed.reshape(packed.shape[0], packed.shape[1], 3, HEADS, HEAD_DIM)
    window_tags = to_windows(jnp.broadcast_to(row_labels[:, None, None], (row_count, col_count, 1)))[:, :, 0]
    allowed = window_tags[:, :, None] == window_tags[:, None, :]
    scores = mixing('wqhd,wkhd->whqk', heads_view[:, :, 0], heads_view[:, :, 1]) * HEAD_DIM ** (-0.5)
    scores = jnp.where(allowed[:, None], scores, masked)
    highest = lax.optimization_barrier(jnp.max(scores, -1, keepdims=True))
    exponent = jnp.exp(scores - highest)
    return (heads_view, exponent / lax.optimization_barrier(jnp.sum(exponent, -1, keepdims=True)))

def window_forward(heads_view, attn_probs, row_count, col_count):
    context = mixing('whqk,wkhd->wqhd', attn_probs.astype(jnp.bfloat16), heads_view[:, :, 2]).astype(jnp.bfloat16)
    return from_windows(context.reshape(context.shape[0], context.shape[1], -1), row_count, col_count)

def window_backward(heads_view, attn_probs, d_context, row_count, col_count):
    probs_low = attn_probs.astype(jnp.bfloat16)
    upstream = to_windows(d_context).reshape(heads_view.shape[0], heads_view.shape[1], HEADS, HEAD_DIM)
    d_probs = mixing('wqhd,wkhd->whqk', upstream, heads_view[:, :, 2])
    d_value = mixing('whqk,wqhd->wkhd', probs_low, upstream)
    d_scores = attn_probs * (d_probs - lax.optimization_barrier(jnp.sum(d_probs * attn_probs, -1, keepdims=True))) * HEAD_DIM ** (-0.5)
    d_scores = d_scores.astype(jnp.bfloat16)
    d_query = mixing('whqk,wkhd->wqhd', d_scores, heads_view[:, :, 1])
    d_key = mixing('whqk,wqhd->wkhd', d_scores, heads_view[:, :, 0])
    joined = jnp.stack([d_query, d_key, d_value], 2).astype(jnp.bfloat16)
    return from_windows(joined.reshape(joined.shape[0], joined.shape[1], -1), row_count, col_count)

def hl_target(bin_index):
    bin_edges = jnp.arange(BINS + 1, dtype=jnp.int32).astype(jnp.float32)
    centre = bin_index.astype(jnp.float32)[..., None] + 0.5
    cumulative = 0.5 * jax.scipy.special.erf((bin_edges - centre) / (smear * math.sqrt(2.0)))
    return (cumulative[..., 1:] - cumulative[..., :-1]) / (cumulative[..., -1:] - cumulative[..., :1])

def head_grad(normed3, w_head, target_bins, land_mask):
    logits = jnp.dot(normed3, w_head, preferred_element_type=jnp.float32).reshape(-1, VARS, BINS)
    highest = lax.optimization_barrier(jnp.max(logits, -1, keepdims=True))
    exponent = jnp.exp(logits - highest)
    bin_probs = exponent / lax.optimization_barrier(jnp.sum(exponent, -1, keepdims=True))
    weight_tok = land_mask.reshape(-1).astype(jnp.float32)[:, None, None] / VARS
    d_logits = weight_tok * (bin_probs - hl_target(target_bins.reshape(-1, VARS)))
    return d_logits.astype(jnp.bfloat16).reshape(-1, VARS * BINS)

def reference(latent, w_qkv, w_proj, w_fc1, w_fc2, w_head, target_bins, land_mask):
    half_rows = WIN_LAT // 2
    half_cols = WIN_LON // 2
    feat_width = latent.shape[-1]
    residual_in = latent.astype(jnp.float32)
    scaled1, inverse1 = normalize(residual_in)
    normed1 = scaled1.astype(jnp.bfloat16)
    shifted = jnp.roll(normed1, (-half_rows, -half_cols), (0, 1))
    qkv_all = jnp.dot(shifted.reshape(-1, feat_width), w_qkv, preferred_element_type=jnp.float32).astype(jnp.bfloat16)
    qkv_rows = qkv_all.reshape(NLAT // WIN_LAT, WIN_LAT, NLON, 3 * feat_width)
    row_labels = (jnp.arange(NLAT, dtype=jnp.int32) + half_rows >= NLAT).astype(jnp.int32)
    label_rows = row_labels.reshape(NLAT // WIN_LAT, WIN_LAT)

    def context_rows(packed_in):
        heads_view, attn_probs = window_setup(packed_in[0], packed_in[1])
        return window_forward(heads_view, attn_probs, WIN_LAT, NLON)
    context = lax.map(context_rows, (qkv_rows, label_rows)).reshape(-1, feat_width)
    attended = jnp.dot(context, w_proj, preferred_element_type=jnp.float32).astype(jnp.bfloat16)
    attended = jnp.roll(attended.reshape(NLAT, NLON, feat_width), (half_rows, half_cols), (0, 1))
    attended = lax.optimization_barrier(attended)
    residual = residual_in + attended.astype(jnp.float32)
    scaled2, inverse2 = normalize(residual)
    normed2 = scaled2.astype(jnp.bfloat16).reshape(-1, feat_width)
    pre_act = jnp.dot(normed2, w_fc1, preferred_element_type=jnp.float32)
    activated, gelu_slope = gelu_parts(pre_act)
    activated = activated.astype(jnp.bfloat16)
    block_out = residual + jnp.dot(activated, w_fc2, preferred_element_type=jnp.float32).reshape(NLAT, NLON, feat_width)
    scaled3, inverse3 = normalize(block_out)
    normed3 = scaled3.astype(jnp.bfloat16).reshape(-1, feat_width)
    d_logits = head_grad(normed3, w_head, target_bins, land_mask)
    grad_head = jnp.dot(normed3.T, d_logits, preferred_element_type=jnp.float32)
    d_out = norm_back(scaled3, inverse3, jnp.dot(d_logits, w_head.T, preferred_element_type=jnp.float32).reshape(NLAT, NLON, feat_width))
    d_outb = d_out.astype(jnp.bfloat16).reshape(-1, feat_width)
    grad_fc2 = jnp.dot(activated.T, d_outb, preferred_element_type=jnp.float32)
    d_pre = (jnp.dot(d_outb, w_fc2.T, preferred_element_type=jnp.float32) * gelu_slope).astype(jnp.bfloat16)
    grad_fc1 = jnp.dot(normed2.T, d_pre, preferred_element_type=jnp.float32)
    d_resid = d_out + norm_back(scaled2, inverse2, jnp.dot(d_pre, w_fc1.T, preferred_element_type=jnp.float32).reshape(NLAT, NLON, feat_width))
    d_attended = jnp.roll(d_resid.astype(jnp.bfloat16), (-half_rows, -half_cols), (0, 1)).reshape(-1, feat_width)
    grad_proj = jnp.dot(context.T, d_attended, preferred_element_type=jnp.float32)
    d_context = jnp.dot(d_attended, w_proj.T, preferred_element_type=jnp.float32).astype(jnp.bfloat16)
    d_context_rows = d_context.reshape(NLAT // WIN_LAT, WIN_LAT, NLON, feat_width)

    def gradient_rows(packed_in):
        heads_view, attn_probs = window_setup(packed_in[0], packed_in[1])
        return window_backward(heads_view, attn_probs, packed_in[2], WIN_LAT, NLON)
    d_qkv = lax.map(gradient_rows, (qkv_rows, label_rows, d_context_rows)).reshape(-1, 3 * feat_width)
    grad_qkv = jnp.dot(shifted.reshape(-1, feat_width).T, d_qkv, preferred_element_type=jnp.float32)
    d_shifted = jnp.dot(d_qkv, w_qkv.T, preferred_element_type=jnp.float32).astype(jnp.bfloat16)
    d_shifted = jnp.roll(d_shifted.reshape(NLAT, NLON, feat_width), (half_rows, half_cols), (0, 1))
    d_shifted = lax.optimization_barrier(d_shifted)
    grad_latent = (d_resid + norm_back(scaled1, inverse1, d_shifted.astype(jnp.float32))).astype(jnp.bfloat16)
    return (grad_latent, grad_qkv, grad_proj, grad_fc1, grad_fc2, grad_head)
```

```python
import math

import jax
import jax.numpy as jnp
from jax import lax
from jax.experimental import pallas as pl
from jax.experimental.pallas import tpu as pltpu
from jax.sharding import Mesh
from jax.sharding import PartitionSpec as P

D = 512
HEADS = 8
FF = 2048
BINS = 256
VARS = 4
WIN_LAT = 6
WIN_LON = 12
HEAD_DIM = 64
TOK = WIN_LAT * WIN_LON
WINDOWS = 12
ROWS = WINDOWS * TOK
CHUNK = 288
WIDE = 640

eps = 1e-05
smear = 0.75
masked = -1e30

LAT = ("x_lo", "z")
LON = ("x_hi", "y", "core")


def normalize(values_in):
    centre = jnp.mean(values_in, -1, keepdims=True)
    offset = values_in - centre
    inverse = lax.rsqrt(jnp.mean(offset * offset, -1, keepdims=True) + eps)
    return (offset * inverse, inverse)


def norm_back(scaled, inverse, upstream):
    return inverse * (
        upstream
        - jnp.mean(upstream, -1, keepdims=True)
        - scaled * jnp.mean(upstream * scaled, -1, keepdims=True)
    )


def gelu_parts(pre_act):
    normal_cdf = 0.5 * (1.0 + lax.erf(pre_act * (1.0 / math.sqrt(2.0))))
    density = jnp.exp(-0.5 * pre_act * pre_act) * (1.0 / math.sqrt(2.0 * math.pi))
    return (pre_act * normal_cdf, normal_cdf + pre_act * density)


def lane_halves(dtype):
    lane = lax.broadcasted_iota(jnp.int32, (1, 2 * HEAD_DIM), 1)
    low = (lane < HEAD_DIM).astype(jnp.float32).astype(dtype)
    return (low, (1 - low).astype(dtype))


def dot_nn(a, b):
    return lax.dot_general(a, b, (((1,), (0,)), ((), ())), preferred_element_type=jnp.float32)


def dot_nt(a, b):
    return lax.dot_general(a, b, (((1,), (1,)), ((), ())), preferred_element_type=jnp.float32)


def dot_tn(a, b):
    return lax.dot_general(a, b, (((0,), (0,)), ((), ())), preferred_element_type=jnp.float32)


def forward_kernel(
    last_ref, xe_ref, sort_ref, wqkv_ref, wproj_ref, wfc1_ref, wfc2_ref, whead_ref,
    qkv_ref, probs_ref, dctx_ref, dres_ref, gwide_ref, gfc2_ref,
    ctx32_ref, ctx_ref, n2_ref, act_ref, slope_ref, dpre_ref, n3_ref, dlog_ref, doutb_ref,
):
    def project(c, carry):
        rows = pl.ds(pl.multiple_of(c * CHUNK, CHUNK), CHUNK)
        scaled, _ = normalize(xe_ref[rows, :D].astype(jnp.float32))
        normed = scaled.astype(jnp.bfloat16)
        for j in range(3):
            part = dot_nn(normed, wqkv_ref[:, j * D : (j + 1) * D])
            for i in range(CHUNK // TOK):
                qkv_ref[c * (CHUNK // TOK) + i, :, j * D : (j + 1) * D] = part[
                    i * TOK : (i + 1) * TOK
                ].astype(jnp.bfloat16)
        return carry

    lax.fori_loop(0, ROWS // CHUNK, project, 0)

    halves = lane_halves(jnp.bfloat16)
    lane = lax.broadcasted_iota(jnp.int32, (TOK, 2 * HEAD_DIM), 1)
    q_late = lax.broadcasted_iota(jnp.int32, (TOK, TOK), 0) >= TOK // 2
    k_late = lax.broadcasted_iota(jnp.int32, (TOK, TOK), 1) >= TOK // 2
    apart = jnp.where(q_late == k_late, 0.0, 1.0)
    last = last_ref[0]

    def attend(w, carry):
        split = jnp.where(jnp.logical_and(last > 0, w >= WINDOWS // 2), 1.0, 0.0)
        block = apart * split
        for pair in range(HEADS // 2):
            at = pair * 2 * HEAD_DIM
            q = qkv_ref[w, :, at : at + 128]
            k = qkv_ref[w, :, D + at : D + at + 128]
            v = qkv_ref[w, :, 2 * D + at : 2 * D + at + 128]
            outs = []
            for e in range(2):
                s = dot_nt(q * halves[e], k) * HEAD_DIM ** (-0.5)
                s = jnp.where(block > 0.5, masked, s)
                ex = jnp.exp(s - jnp.max(s, -1, keepdims=True))
                p = ex / jnp.sum(ex, -1, keepdims=True)
                low = p.astype(jnp.bfloat16)
                probs_ref[w, 2 * pair + e] = low
                outs.append(dot_nn(low, v))
            ctx32_ref[pl.ds(pl.multiple_of(w * TOK, 8), TOK), at : at + 128] = jnp.where(
                lane < HEAD_DIM, outs[0], outs[1]
            )
        return carry

    lax.fori_loop(0, WINDOWS, attend, 0)

    edge = lax.broadcasted_iota(jnp.int32, (1, BINS), 1).astype(jnp.float32)
    width = 1.0 / (smear * math.sqrt(2.0))

    def dense(c, carry):
        rows = pl.ds(pl.multiple_of(c * CHUNK, CHUNK), CHUNK)
        ctx = ctx32_ref[rows, :].astype(jnp.bfloat16)
        ctx_ref[rows, :] = dot_nn(ctx, sort_ref[...]).astype(jnp.bfloat16)
        attended = dot_nn(ctx, wproj_ref[...]).astype(jnp.bfloat16)
        residual = xe_ref[rows, :D].astype(jnp.float32) + attended.astype(jnp.float32)
        scaled2, inverse2 = normalize(residual)
        n2 = scaled2.astype(jnp.bfloat16)
        n2_ref[rows, :] = dot_nn(n2, sort_ref[...]).astype(jnp.bfloat16)
        out = residual
        for j in range(FF // D):
            cols = slice(j * D, (j + 1) * D)
            act, slope = gelu_parts(dot_nn(n2, wfc1_ref[:, cols]))
            act = act.astype(jnp.bfloat16)
            act_ref[rows, cols] = act
            slope_ref[:, cols] = slope
            out = out + dot_nn(act, wfc2_ref[cols, :])
        scaled3, inverse3 = normalize(out)
        n3 = scaled3.astype(jnp.bfloat16)
        n3_ref[rows, :] = dot_nn(n3, sort_ref[...]).astype(jnp.bfloat16)
        extra = xe_ref[rows, D : D + 128].astype(jnp.float32)
        weight = extra[:, VARS : VARS + 1] / VARS
        dz = jnp.zeros((CHUNK, D), jnp.float32)
        for v in range(VARS):
            cols = slice(v * BINS, (v + 1) * BINS)
            logits = dot_nn(n3, whead_ref[:, cols])
            ex = jnp.exp(logits - jnp.max(logits, -1, keepdims=True))
            probs = ex / jnp.sum(ex, -1, keepdims=True)
            centre = extra[:, v : v + 1] + 0.5
            mass = lax.erf((edge + 1.0 - centre) * width) - lax.erf((edge - centre) * width)
            total = lax.erf((BINS - centre) * width) - lax.erf((0.0 - centre) * width)
            d_log = (weight * (probs - mass / total)).astype(jnp.bfloat16)
            dlog_ref[rows, cols] = d_log
            dz = dz + dot_nt(d_log, whead_ref[:, cols])
        d_out = norm_back(scaled3, inverse3, dz)
        d_outb = d_out.astype(jnp.bfloat16)
        doutb_ref[rows, :] = d_outb
        dn = jnp.zeros((CHUNK, D), jnp.float32)
        for j in range(FF // D):
            cols = slice(j * D, (j + 1) * D)
            d_pre = (dot_nt(d_outb, wfc2_ref[cols, :]) * slope_ref[:, cols]).astype(jnp.bfloat16)
            dpre_ref[rows, cols] = d_pre
            dn = dn + dot_nt(d_pre, wfc1_ref[:, cols])
        d_res = d_out + norm_back(scaled2, inverse2, dn)
        dres_ref[rows, :] = d_res
        d_ctx = dot_nt(d_res.astype(jnp.bfloat16), wproj_ref[...])
        for i in range(CHUNK // TOK):
            dctx_ref[c * (CHUNK // TOK) + i] = d_ctx[i * TOK : (i + 1) * TOK].astype(jnp.bfloat16)
        return carry

    lax.fori_loop(0, ROWS // CHUNK, dense, 0)

    for j in range(2):
        cols = slice(j * D, (j + 1) * D)
        gwide_ref[:, cols] = dot_tn(n3_ref[...], dlog_ref[:, cols]).astype(jnp.bfloat16)
    for j in range(FF // D):
        cols = slice(j * D, (j + 1) * D)
        gfc2_ref[cols, :] = dot_tn(act_ref[:, cols], doutb_ref[...]).astype(jnp.bfloat16)
        gwide_ref[:, 2 * D + j * D : 3 * D + j * D] = dot_tn(n2_ref[...], dpre_ref[:, cols]).astype(
            jnp.bfloat16
        )
    gwide_ref[:, 6 * D :] = dot_tn(ctx_ref[...], dres_ref[...].astype(jnp.bfloat16)).astype(
        jnp.bfloat16
    )


def backward_kernel(
    xe_ref, sort_ref, qkv_ref, probs_ref, dctx_ref, dres_ref, wqkv_ref,
    glat_ref, gqkv_ref,
    dqkv32_ref, dqkv_ref, n1_ref,
):
    halves = lane_halves(jnp.bfloat16)
    lane = lax.broadcasted_iota(jnp.int32, (TOK, 2 * HEAD_DIM), 1)
    lower = lane < HEAD_DIM

    def attend(w, carry):
        rows = pl.ds(pl.multiple_of(w * TOK, 8), TOK)
        for pair in range(HEADS // 2):
            at = pair * 2 * HEAD_DIM
            q = qkv_ref[w, :, at : at + 128]
            k = qkv_ref[w, :, D + at : D + at + 128]
            v = qkv_ref[w, :, 2 * D + at : 2 * D + at + 128]
            up = dctx_ref[w, :, at : at + 128]
            dq, dk, dv = ([], [], [])
            for e in range(2):
                low = probs_ref[w, 2 * pair + e]
                p = low.astype(jnp.float32)
                d_p = dot_nt(up * halves[e], v)
                d_s = p * (d_p - jnp.sum(d_p * p, -1, keepdims=True)) * HEAD_DIM ** (-0.5)
                d_s = d_s.astype(jnp.bfloat16)
                dv.append(dot_tn(low, up))
                dq.append(dot_nn(d_s, k))
                dk.append(dot_tn(d_s, q))
            dqkv32_ref[rows, at : at + 128] = jnp.where(lower, dq[0], dq[1])
            dqkv32_ref[rows, D + at : D + at + 128] = jnp.where(lower, dk[0], dk[1])
            dqkv32_ref[rows, 2 * D + at : 2 * D + at + 128] = jnp.where(lower, dv[0], dv[1])
        return carry

    lax.fori_loop(0, WINDOWS, attend, 0)

    def finish(c, carry):
        rows = pl.ds(pl.multiple_of(c * CHUNK, CHUNK), CHUNK)
        scaled1, inverse1 = normalize(xe_ref[rows, :D].astype(jnp.float32))
        n1_ref[rows, :] = dot_nn(scaled1.astype(jnp.bfloat16), sort_ref[...]).astype(jnp.bfloat16)
        d_qkv = dqkv32_ref[rows, :].astype(jnp.bfloat16)
        dqkv_ref[rows, :] = d_qkv
        d_sh = dot_nt(d_qkv, wqkv_ref[...]).astype(jnp.bfloat16).astype(jnp.float32)
        glat_ref[rows, :] = (dres_ref[rows, :] + norm_back(scaled1, inverse1, d_sh)).astype(
            jnp.bfloat16
        )
        return carry

    lax.fori_loop(0, ROWS // CHUNK, finish, 0)
    for j in range(3):
        cols = slice(j * D, (j + 1) * D)
        gqkv_ref[:, cols] = dot_tn(n1_ref[...], dqkv_ref[:, cols]).astype(jnp.bfloat16)


def whole(shape, dtype):
    return jax.ShapeDtypeStruct(shape, dtype)


VMEM_SPEC = pl.BlockSpec(memory_space=pltpu.VMEM)


def run_forward(last, xe, sort, w_qkv, w_proj, w_fc1, w_fc2, w_head):
    bf, f32 = (jnp.bfloat16, jnp.float32)
    return pl.pallas_call(
        forward_kernel,
        out_shape=(
            whole((WINDOWS, TOK, 3 * D), bf),
            whole((WINDOWS, HEADS, TOK, TOK), bf),
            whole((WINDOWS, TOK, D), bf),
            whole((ROWS, D), f32),
            whole((D, 7 * D), bf),
            whole((FF, D), bf),
        ),
        in_specs=[pl.BlockSpec(memory_space=pltpu.SMEM)] + [VMEM_SPEC] * 7,
        out_specs=(VMEM_SPEC,) * 6,
        scratch_shapes=[
            pltpu.VMEM((ROWS, D), f32),
            pltpu.VMEM((ROWS, D), bf),
            pltpu.VMEM((ROWS, D), bf),
            pltpu.VMEM((ROWS, FF), bf),
            pltpu.VMEM((CHUNK, FF), f32),
            pltpu.VMEM((ROWS, FF), bf),
            pltpu.VMEM((ROWS, D), bf),
            pltpu.VMEM((ROWS, VARS * BINS), bf),
            pltpu.VMEM((ROWS, D), bf),
        ],
        compiler_params=pltpu.CompilerParams(vmem_limit_bytes=60 * 1024 * 1024),
        name="forward",
    )(last, xe, sort, w_qkv, w_proj, w_fc1, w_fc2, w_head)


def run_backward(xe, sort, qkv, probs, d_ctx, d_res, w_qkv):
    bf, f32 = (jnp.bfloat16, jnp.float32)
    return pl.pallas_call(
        backward_kernel,
        out_shape=(whole((ROWS, D), bf), whole((D, 3 * D), bf)),
        in_specs=[VMEM_SPEC] * 7,
        out_specs=(VMEM_SPEC,) * 2,
        scratch_shapes=[
            pltpu.VMEM((ROWS, 3 * D), f32),
            pltpu.VMEM((ROWS, 3 * D), bf),
            pltpu.VMEM((ROWS, D), bf),
        ],
        compiler_params=pltpu.CompilerParams(vmem_limit_bytes=60 * 1024 * 1024),
        name="backward",
    )(xe, sort, qkv, probs, d_ctx, d_res, w_qkv)


def sorter():
    source = lax.broadcasted_iota(jnp.int32, (D, D), 0)
    target = lax.broadcasted_iota(jnp.int32, (D, D), 1)
    wanted = (target % 256) // 4 * 8 + (target // 256) * 4 + target % 4
    return (source == wanted).astype(jnp.bfloat16)


def ring_pairs(axes, step):
    if isinstance(axes, str):
        return [(i, (i + step) % 4) for i in range(4)]
    place = [(i % 2) * 2 + i // 2 for i in range(4)]
    return [(place[i], place[(i + step) % 4]) for i in range(4)]


def position(axes):
    if isinstance(axes, str):
        return lax.axis_index(axes)
    return lax.axis_index("x_hi") * 2 + lax.axis_index("x_lo")


X = ("x_lo", "x_hi")


def pick(value, axes, dims, at):
    if isinstance(axes, str):
        return lax.dynamic_index_in_dim(value, at, dims[0], False)
    value = lax.dynamic_index_in_dim(value, at // 2, dims[1], False)
    return lax.dynamic_index_in_dim(value, at % 2, dims[0], False)


def ring_sum(value, axes, dims, last=False):
    me = position(axes)
    total = pick(value, axes, dims, me).astype(jnp.float32)
    arrived = [
        lax.ppermute(pick(value, axes, dims, (me + step) % 4), axes, ring_pairs(axes, step))
        for step in (2, 1, 3)
    ]
    for part in arrived:
        total = total + part.astype(jnp.float32)
    return total if last else total.astype(jnp.bfloat16)


def core_sum(value, dim):
    me = lax.axis_index("core")
    other = lax.ppermute(
        lax.dynamic_index_in_dim(value, 1 - me, dim, False), "core", [(0, 1), (1, 0)]
    )
    mine = lax.dynamic_index_in_dim(value, me, dim, False)
    return (mine.astype(jnp.float32) + other.astype(jnp.float32)).astype(jnp.bfloat16)


def reduce_wide(value, x_first):
    n = value.shape[1]
    value = core_sum(value.reshape(2, 2, 4, 2, 16, n), 0)
    if x_first:
        value = ring_sum(ring_sum(value, X, (0, 2)), "z", (0,))
    else:
        value = ring_sum(ring_sum(value, "z", (1,)), X, (0, 1))
    return ring_sum(value.reshape(4, 4, n), "y", (0,), True)


def reduce_tall(value):
    value = core_sum(value.reshape(2, 4, 2, 4, 2, 16, D), 4)
    value = ring_sum(ring_sum(value, X, (0, 2)), "z", (0,))
    return ring_sum(value, "y", (0,), True)


def shifted_2(value, axis, steps):
    count = lax.axis_size(axis)
    pairs = [(source, (source + steps) % count) for source in range(count)]
    return lax.ppermute(value, axis, pairs)


def local(latent, w_qkv, w_proj, w_fc1, w_fc2, w_head, target_bins, land_mask):
    row_count, col_count, _ = latent.shape
    half_rows = WIN_LAT // 2
    half_cols = WIN_LON // 2
    bf = jnp.bfloat16
    ext = jnp.concatenate(
        [
            latent,
            target_bins.astype(bf),
            land_mask[:, :, None].astype(bf),
            jnp.zeros((row_count, col_count, WIDE - D - VARS - 1), bf),
        ],
        2,
    )
    edge_cols = shifted_2(ext[:, :half_cols], LON, -1)
    moved = jnp.concatenate([ext[:, half_cols:], edge_cols], 1)
    edge_rows = shifted_2(moved[:half_rows], LAT, -1)
    block = jnp.concatenate([moved[half_rows:], edge_rows], 0)
    shaped = block.reshape(row_count // WIN_LAT, WIN_LAT, col_count // WIN_LON, WIN_LON, WIDE)
    xe = shaped.transpose(0, 2, 1, 3, 4).reshape(ROWS, WIDE)
    last = (lax.axis_index(LAT) == lax.axis_size(LAT) - 1).astype(jnp.int32).reshape(1)
    sort = sorter()
    qkv, probs, d_ctx, d_res, g_wide, g_tall = run_forward(
        last, xe, sort, w_qkv, w_proj, w_fc1, w_fc2, w_head
    )
    grad_latent, g_qkv = run_backward(xe, sort, qkv, probs, d_ctx, d_res, w_qkv)
    shaped = grad_latent.reshape(
        row_count // WIN_LAT, col_count // WIN_LON, WIN_LAT, WIN_LON, D
    )
    grad_latent = shaped.transpose(0, 2, 1, 3, 4).reshape(row_count, col_count, D)
    grad_cols = shifted_2(grad_latent[:, col_count - half_cols :], LON, 1)
    grad_moved = jnp.concatenate([grad_cols, grad_latent[:, : col_count - half_cols]], 1)
    grad_rows = shifted_2(grad_moved[row_count - half_rows :], LAT, 1)
    grad_latent = jnp.concatenate([grad_rows, grad_moved[: row_count - half_rows]], 0)
    wide = reduce_wide(g_wide, False)
    tall = reduce_tall(g_tall)
    qkv_part = reduce_wide(g_qkv, False)
    return (
        grad_latent,
        qkv_part,
        wide[:, 6 * D :],
        wide[:, 2 * D : 6 * D],
        tall,
        wide[:, : 2 * D],
    )


def solution(mesh):
    fine = Mesh(mesh.devices.reshape(2, 4, 2, 4, 2), LAT + LON)
    grid = P(LAT, LON)
    rows = P(LAT + LON, None)
    return jax.shard_map(
        local,
        mesh=fine,
        in_specs=(P(LAT, LON, None), P(), P(), P(), P(), P(), P(LAT, LON, None), grid),
        out_specs=(P(LAT, LON, None), rows, rows, rows, rows, rows),
        check_vma=False,
    )
```

```python
import math

import jax
import jax.numpy as jnp
from jax import lax
from jax.experimental import pallas as pl
from jax.experimental.pallas import tpu as pltpu
from jax.sharding import Mesh
from jax.sharding import PartitionSpec as P

D = 512
HEADS = 8
FF = 2048
BINS = 256
VARS = 4
WIN_LAT = 6
WIN_LON = 12
HEAD_DIM = 64
TOK = WIN_LAT * WIN_LON
WINDOWS = 12
ROWS = WINDOWS * TOK
CHUNK = 288
WIDE = 640

eps = 1e-05
smear = 0.75
masked = -1e30

LAT = ("x_lo", "z")
LON = ("x_hi", "y", "core")


def normalize(values_in):
    centre = jnp.mean(values_in, -1, keepdims=True)
    offset = values_in - centre
    inverse = lax.rsqrt(jnp.mean(offset * offset, -1, keepdims=True) + eps)
    return (offset * inverse, inverse)


def norm_back(scaled, inverse, upstream):
    return inverse * (
        upstream
        - jnp.mean(upstream, -1, keepdims=True)
        - scaled * jnp.mean(upstream * scaled, -1, keepdims=True)
    )


def gelu_parts(pre_act):
    normal_cdf = 0.5 * (1.0 + lax.erf(pre_act * (1.0 / math.sqrt(2.0))))
    density = jnp.exp(-0.5 * pre_act * pre_act) * (1.0 / math.sqrt(2.0 * math.pi))
    return (pre_act * normal_cdf, normal_cdf + pre_act * density)


def lane_halves(dtype):
    lane = lax.broadcasted_iota(jnp.int32, (1, 2 * HEAD_DIM), 1)
    low = (lane < HEAD_DIM).astype(jnp.float32).astype(dtype)
    return (low, (1 - low).astype(dtype))


def dot_nn(a, b):
    return lax.dot_general(a, b, (((1,), (0,)), ((), ())), preferred_element_type=jnp.float32)


def dot_nt(a, b):
    return lax.dot_general(a, b, (((1,), (1,)), ((), ())), preferred_element_type=jnp.float32)


def forward_kernel(
    at_ref, xe_ref, sort_ref, sort_tall_ref, wqkv_ref, wproj_ref, wfc1_ref, wfc2_ref, whead_ref,
    qkv_ref, probs_ref, probs_t_ref, dctx_ref, dres_ref, gown_ref, gother_ref,
    ctx32_ref, ctx_ref, n2_ref, act_ref, slope_ref, dpre_ref, n3_ref, dlog_ref, doutb_ref, left_ref,
):
    def project(c, carry):
        rows = pl.ds(pl.multiple_of(c * CHUNK, CHUNK), CHUNK)
        scaled, _ = normalize(xe_ref[rows, :D].astype(jnp.float32))
        normed = scaled.astype(jnp.bfloat16)
        for j in range(3):
            part = dot_nn(normed, wqkv_ref[:, j * D : (j + 1) * D])
            for i in range(CHUNK // TOK):
                qkv_ref[c * (CHUNK // TOK) + i, :, j * D : (j + 1) * D] = part[
                    i * TOK : (i + 1) * TOK
                ].astype(jnp.bfloat16)
        return carry

    lax.fori_loop(0, ROWS // CHUNK, project, 0)

    halves = lane_halves(jnp.bfloat16)
    lane = lax.broadcasted_iota(jnp.int32, (TOK, 2 * HEAD_DIM), 1)
    q_late = lax.broadcasted_iota(jnp.int32, (TOK, TOK), 0) >= TOK // 2
    k_late = lax.broadcasted_iota(jnp.int32, (TOK, TOK), 1) >= TOK // 2
    apart = jnp.where(q_late == k_late, 0.0, 1.0)
    last = at_ref[3]

    def attend(w, carry):
        split = jnp.where(jnp.logical_and(last > 0, w >= WINDOWS // 2), 1.0, 0.0)
        block = apart * split
        for pair in range(HEADS // 2):
            at = pair * 2 * HEAD_DIM
            q = qkv_ref[w, :, at : at + 128]
            k = qkv_ref[w, :, D + at : D + at + 128]
            v = qkv_ref[w, :, 2 * D + at : 2 * D + at + 128]
            outs = []
            for e in range(2):
                one = q * halves[e]
                s = dot_nt(one, k) * HEAD_DIM ** (-0.5)
                s = jnp.where(block > 0.5, masked, s)
                ex = jnp.exp(s - jnp.max(s, -1, keepdims=True))
                low = (ex / jnp.sum(ex, -1, keepdims=True)).astype(jnp.bfloat16)
                probs_ref[w, 2 * pair + e] = low
                s = dot_nt(k, one) * HEAD_DIM ** (-0.5)
                s = jnp.where(block > 0.5, masked, s)
                ex = jnp.exp(s - jnp.max(s, 0, keepdims=True))
                probs_t_ref[w, 2 * pair + e] = (ex / jnp.sum(ex, 0, keepdims=True)).astype(
                    jnp.bfloat16
                )
                outs.append(dot_nn(low, v))
            ctx32_ref[pl.ds(pl.multiple_of(w * TOK, 8), TOK), at : at + 128] = jnp.where(
                lane < HEAD_DIM, outs[0], outs[1]
            )
        return carry

    lax.fori_loop(0, WINDOWS, attend, 0)

    edge = lax.broadcasted_iota(jnp.int32, (1, BINS), 1).astype(jnp.float32)
    width = 1.0 / (smear * math.sqrt(2.0))

    def dense(c, carry):
        rows = pl.ds(pl.multiple_of(c * CHUNK, CHUNK), CHUNK)
        ctx = ctx32_ref[rows, :].astype(jnp.bfloat16)
        ctx_ref[rows, :] = ctx
        attended = dot_nn(ctx, wproj_ref[...]).astype(jnp.bfloat16)
        residual = xe_ref[rows, :D].astype(jnp.float32) + attended.astype(jnp.float32)
        scaled2, inverse2 = normalize(residual)
        n2 = scaled2.astype(jnp.bfloat16)
        n2_ref[rows, :] = n2
        out = residual
        for j in range(FF // D):
            cols = slice(j * D, (j + 1) * D)
            act, slope = gelu_parts(dot_nn(n2, wfc1_ref[:, cols]))
            act = act.astype(jnp.bfloat16)
            act_ref[rows, cols] = act
            slope_ref[:, cols] = slope
            out = out + dot_nn(act, wfc2_ref[cols, :])
        scaled3, inverse3 = normalize(out)
        n3 = scaled3.astype(jnp.bfloat16)
        n3_ref[rows, :] = n3
        extra = xe_ref[rows, D : D + 128].astype(jnp.float32)
        weight = extra[:, VARS : VARS + 1] / VARS
        dz = jnp.zeros((CHUNK, D), jnp.float32)
        for v in range(VARS):
            cols = slice(v * BINS, (v + 1) * BINS)
            logits = dot_nn(n3, whead_ref[:, cols])
            ex = jnp.exp(logits - jnp.max(logits, -1, keepdims=True))
            probs = ex / jnp.sum(ex, -1, keepdims=True)
            centre = extra[:, v : v + 1] + 0.5
            mass = lax.erf((edge + 1.0 - centre) * width) - lax.erf((edge - centre) * width)
            total = lax.erf((BINS - centre) * width) - lax.erf((0.0 - centre) * width)
            d_log = (weight * (probs - mass / total)).astype(jnp.bfloat16)
            dlog_ref[rows, cols] = d_log
            dz = dz + dot_nt(d_log, whead_ref[:, cols])
        d_out = norm_back(scaled3, inverse3, dz)
        d_outb = d_out.astype(jnp.bfloat16)
        doutb_ref[rows, :] = d_outb
        dn = jnp.zeros((CHUNK, D), jnp.float32)
        for j in range(FF // D):
            cols = slice(j * D, (j + 1) * D)
            d_pre = (dot_nt(d_outb, wfc2_ref[cols, :]) * slope_ref[:, cols]).astype(jnp.bfloat16)
            dpre_ref[rows, cols] = d_pre
            dn = dn + dot_nt(d_pre, wfc1_ref[:, cols])
        d_res = d_out + norm_back(scaled2, inverse2, dn)
        dres_ref[rows, :] = d_res
        d_ctx = dot_nt(d_res.astype(jnp.bfloat16), wproj_ref[...])
        for i in range(CHUNK // TOK):
            dctx_ref[c * (CHUNK // TOK) + i] = d_ctx[i * TOK : (i + 1) * TOK].astype(jnp.bfloat16)
        return carry

    lax.fori_loop(0, ROWS // CHUNK, dense, 0)

    def keep(at, grad):
        gown_ref[:, at : at + D] = grad[: D // 2].astype(jnp.bfloat16)
        gother_ref[:, at : at + D] = grad[D // 2 :].astype(jnp.bfloat16)

    def turned(one_hot, value):
        left_ref[...] = dot_nt(one_hot, value).astype(jnp.bfloat16)

    turned(sort_ref[...], n3_ref[...])
    for j in range(2):
        keep(j * D, dot_nn(left_ref[...], dlog_ref[:, j * D : (j + 1) * D]))
    turned(sort_ref[...], n2_ref[...])
    for j in range(FF // D):
        cols = slice(j * D, (j + 1) * D)
        keep(2 * D + j * D, dot_nn(left_ref[...], dpre_ref[:, cols]))
    turned(sort_ref[...], ctx_ref[...])
    keep(6 * D, dot_nn(left_ref[...], dres_ref[...].astype(jnp.bfloat16)))
    for m in range(FF // D):
        turned(sort_tall_ref[...], act_ref[:, m * D : (m + 1) * D])
        grad = dot_nn(left_ref[...], doutb_ref[...]).astype(jnp.bfloat16)
        for t in range(32):
            i1, core, z_low, x_hi = (t // 8, t // 4 % 2, t // 2 % 2, t % 2)
            z = (m % 2 * 2 + z_low + 4 - at_ref[2]) % 4
            x = (x_hi * 2 + m // 2 + 4 - at_ref[0]) % 4
            rows = pl.ds(pl.multiple_of(z * 64 + x * 16, 16), 16)
            target = gother_ref if core else gown_ref
            target[rows, 7 * D + i1 * D : 8 * D + i1 * D] = grad[t * 16 : (t + 1) * 16]


def attention_back_kernel(
    qkv_ref, probs_ref, probs_t_ref, dctx_ref, dqkv_ref, dqkv32_ref
):
    halves = lane_halves(jnp.bfloat16)
    lane = lax.broadcasted_iota(jnp.int32, (TOK, 2 * HEAD_DIM), 1)
    lower = lane < HEAD_DIM

    def attend(w, carry):
        rows = pl.ds(pl.multiple_of(w * TOK, 8), TOK)
        for pair in range(HEADS // 2):
            at = pair * 2 * HEAD_DIM
            q = qkv_ref[w, :, at : at + 128]
            k = qkv_ref[w, :, D + at : D + at + 128]
            v = qkv_ref[w, :, 2 * D + at : 2 * D + at + 128]
            up = dctx_ref[w, :, at : at + 128]
            dq, dk, dv = ([], [], [])
            for e in range(2):
                one = up * halves[e]
                p = probs_ref[w, 2 * pair + e].astype(jnp.float32)
                d_p = dot_nt(one, v)
                d_s = p * (d_p - jnp.sum(d_p * p, -1, keepdims=True)) * HEAD_DIM ** (-0.5)
                dq.append(dot_nn(d_s.astype(jnp.bfloat16), k))
                low = probs_t_ref[w, 2 * pair + e]
                p = low.astype(jnp.float32)
                d_p = dot_nt(v, one)
                d_s = p * (d_p - jnp.sum(d_p * p, 0, keepdims=True)) * HEAD_DIM ** (-0.5)
                dk.append(dot_nn(d_s.astype(jnp.bfloat16), q))
                dv.append(dot_nn(low, up))
            dqkv32_ref[rows, at : at + 128] = jnp.where(lower, dq[0], dq[1])
            dqkv32_ref[rows, D + at : D + at + 128] = jnp.where(lower, dk[0], dk[1])
            dqkv32_ref[rows, 2 * D + at : 2 * D + at + 128] = jnp.where(lower, dv[0], dv[1])
        return carry

    lax.fori_loop(0, WINDOWS // 2, attend, 0)
    dqkv_ref[...] = dqkv32_ref[...].astype(jnp.bfloat16)


def finish_kernel(
    xe_ref, sort_ref, dqkv_a_ref, dqkv_b_ref, dres_ref, wqkv_ref,
    glat_ref, gown_ref, gother_ref,
    n1_ref,
):
    half = ROWS // 2
    for c, dqkv_ref in enumerate((dqkv_a_ref, dqkv_b_ref)):
        rows = slice(c * half, (c + 1) * half)
        scaled1, inverse1 = normalize(xe_ref[rows, :D].astype(jnp.float32))
        n1_ref[c] = dot_nt(sort_ref[...], scaled1.astype(jnp.bfloat16)).astype(jnp.bfloat16)
        d_sh = dot_nt(dqkv_ref[...], wqkv_ref[...]).astype(jnp.bfloat16).astype(jnp.float32)
        glat_ref[rows, :] = (dres_ref[rows, :] + norm_back(scaled1, inverse1, d_sh)).astype(
            jnp.bfloat16
        )
    for j in range(3):
        cols = slice(j * D, (j + 1) * D)
        grad = dot_nn(n1_ref[0], dqkv_a_ref[:, cols]) + dot_nn(n1_ref[1], dqkv_b_ref[:, cols])
        gown_ref[:, cols] = grad[: D // 2].astype(jnp.bfloat16)
        gother_ref[:, cols] = grad[D // 2 :].astype(jnp.bfloat16)


def whole(shape, dtype):
    return jax.ShapeDtypeStruct(shape, dtype)


VMEM_SPEC = pl.BlockSpec(memory_space=pltpu.VMEM)


def run_forward(at, xe, sort, sort_tall, w_qkv, w_proj, w_fc1, w_fc2, w_head):
    bf, f32 = (jnp.bfloat16, jnp.float32)
    return pl.pallas_call(
        forward_kernel,
        out_shape=(
            whole((WINDOWS, TOK, 3 * D), bf),
            whole((WINDOWS, HEADS, TOK, TOK), bf),
            whole((WINDOWS, HEADS, TOK, TOK), bf),
            whole((WINDOWS, TOK, D), bf),
            whole((ROWS, D), f32),
            whole((D // 2, 11 * D), bf),
            whole((D // 2, 11 * D), bf),
        ),
        in_specs=[pl.BlockSpec(memory_space=pltpu.SMEM)] + [VMEM_SPEC] * 8,
        out_specs=(VMEM_SPEC,) * 7,
        scratch_shapes=[
            pltpu.VMEM((ROWS, D), f32),
            pltpu.VMEM((ROWS, D), bf),
            pltpu.VMEM((ROWS, D), bf),
            pltpu.VMEM((ROWS, FF), bf),
            pltpu.VMEM((CHUNK, FF), f32),
            pltpu.VMEM((ROWS, FF), bf),
            pltpu.VMEM((ROWS, D), bf),
            pltpu.VMEM((ROWS, VARS * BINS), bf),
            pltpu.VMEM((ROWS, D), bf),
            pltpu.VMEM((D, ROWS), bf),
        ],
        compiler_params=pltpu.CompilerParams(vmem_limit_bytes=60 * 1024 * 1024),
        name="forward",
    )(at, xe, sort, sort_tall, w_qkv, w_proj, w_fc1, w_fc2, w_head)


def run_attention_back(part, qkv, probs, probs_t, d_ctx):
    bf, f32 = (jnp.bfloat16, jnp.float32)
    half = WINDOWS // 2
    return pl.pallas_call(
        attention_back_kernel,
        out_shape=whole((ROWS // 2, 3 * D), bf),
        grid=(1,),
        in_specs=[
            pl.BlockSpec((half, TOK, 3 * D), lambda i: (part, 0, 0)),
            pl.BlockSpec((half, HEADS, TOK, TOK), lambda i: (part, 0, 0, 0)),
            pl.BlockSpec((half, HEADS, TOK, TOK), lambda i: (part, 0, 0, 0)),
            pl.BlockSpec((half, TOK, D), lambda i: (part, 0, 0)),
        ],
        out_specs=pl.BlockSpec((ROWS // 2, 3 * D), lambda i: (0, 0)),
        scratch_shapes=[pltpu.VMEM((ROWS // 2, 3 * D), f32)],
        compiler_params=pltpu.CompilerParams(vmem_limit_bytes=48 * 1024 * 1024),
        name="attention_back",
        cost_estimate=pl.CostEstimate(
            flops=10**9, transcendentals=0, bytes_accessed=4 * 10**6
        ),
    )(qkv, probs, probs_t, d_ctx)


def run_finish(xe, sort, dqkv_a, dqkv_b, d_res, w_qkv):
    bf = jnp.bfloat16
    return pl.pallas_call(
        finish_kernel,
        out_shape=(
            whole((ROWS, D), bf),
            whole((D // 2, 3 * D), bf),
            whole((D // 2, 3 * D), bf),
        ),
        in_specs=[VMEM_SPEC] * 6,
        out_specs=(VMEM_SPEC,) * 3,
        scratch_shapes=[pltpu.VMEM((2, D, ROWS // 2), bf)],
        compiler_params=pltpu.CompilerParams(vmem_limit_bytes=48 * 1024 * 1024),
        name="finish",
        cost_estimate=pl.CostEstimate(
            flops=10**9, transcendentals=0, bytes_accessed=8 * 10**6
        ),
    )(xe, sort, dqkv_a, dqkv_b, d_res, w_qkv)


def place():
    x = lax.axis_index("x_hi") * 2 + lax.axis_index("x_lo")
    return (x, lax.axis_index("y"), lax.axis_index("z"), lax.axis_index("core"))


def sorter():
    x_me, y_me, z_me, core_me = place()
    at = lax.broadcasted_iota(jnp.int32, (D, 1), 0)
    source = lax.broadcasted_iota(jnp.int32, (D, D), 1)
    core = (at // 256 + core_me) % 2
    z = (at // 64 + z_me) % 4
    x = (at // 16 + x_me) % 4
    y = (at // 4 + y_me) % 4
    owner = ((((x % 2) * 4 + z) * 2 + x // 2) * 4 + y) * 2 + core
    return (source == owner * 4 + at % 4).astype(jnp.bfloat16)


def tall_sorter():
    _, y_me, _, core_me = place()
    at = lax.broadcasted_iota(jnp.int32, (D, 1), 0)
    source = lax.broadcasted_iota(jnp.int32, (D, D), 1)
    core = (at // 64 + core_me) % 2
    y = (at // 4 + y_me) % 4
    owner = (at // 16 % 4 * 4 + y) * 2 + core
    return (source == owner * 16 + at // 128 * 4 + at % 4).astype(jnp.bfloat16)


def ring_pairs(axes, step):
    if isinstance(axes, str):
        return [(i, (i + step) % 4) for i in range(4)]
    spot = [(i % 2) * 2 + i // 2 for i in range(4)]
    return [(spot[i], spot[(i + step) % 4]) for i in range(4)]


X = ("x_lo", "x_hi")


def add_up(own, arrived, last=False):
    total = own.astype(jnp.float32)
    for part in arrived:
        total = total + part.astype(jnp.float32)
    return total if last else total.astype(jnp.bfloat16)


def ring_send(blocks, axes):
    return (
        blocks[0],
        [lax.ppermute(blocks[s], axes, ring_pairs(axes, s)) for s in (2, 1, 3)],
    )


def quarters(value):
    n = value.shape[0] // 4
    return [value[i * n : (i + 1) * n] for i in range(4)]


def core_send(value):
    return lax.ppermute(value, "core", [(0, 1), (1, 0)])


def shifted_2(value, axis, steps):
    count = lax.axis_size(axis)
    pairs = [(source, (source + steps) % count) for source in range(count)]
    return lax.ppermute(value, axis, pairs)


def local(latent, w_qkv, w_proj, w_fc1, w_fc2, w_head, target_bins, land_mask):
    row_count, col_count, _ = latent.shape
    half_rows = WIN_LAT // 2
    half_cols = WIN_LON // 2
    bf = jnp.bfloat16
    ext = jnp.concatenate(
        [
            latent,
            target_bins.astype(bf),
            land_mask[:, :, None].astype(bf),
            jnp.zeros((row_count, col_count, WIDE - D - VARS - 1), bf),
        ],
        2,
    )
    edge_cols = shifted_2(ext[:, :half_cols], LON, -1)
    moved = jnp.concatenate([ext[:, half_cols:], edge_cols], 1)
    edge_rows = shifted_2(moved[:half_rows], LAT, -1)
    block = jnp.concatenate([moved[half_rows:], edge_rows], 0)
    shaped = block.reshape(row_count // WIN_LAT, WIN_LAT, col_count // WIN_LON, WIN_LON, WIDE)
    xe = shaped.transpose(0, 2, 1, 3, 4).reshape(ROWS, WIDE)
    last = (lax.axis_index(LAT) == lax.axis_size(LAT) - 1).astype(jnp.int32)
    x_me, y_me, z_me, _ = place()
    at = jnp.stack([x_me, y_me, z_me, last])
    sort = sorter()
    qkv, probs, probs_t, d_ctx, d_res, wide_own, wide_other = run_forward(
        at, xe, sort, tall_sorter(), w_qkv, w_proj, w_fc1, w_fc2, w_head
    )
    wide_got = core_send(wide_other)
    d_qkv_a = run_attention_back(0, qkv, probs, probs_t, d_ctx)
    wide = ring_send(quarters(add_up(wide_own, [wide_got])), "z")
    d_qkv_b = run_attention_back(1, qkv, probs, probs_t, d_ctx)
    grad_latent, qkv_own, qkv_other = run_finish(xe, sort, d_qkv_a, d_qkv_b, d_res, w_qkv)
    qkv_got = core_send(qkv_other)
    part = add_up(qkv_own, [qkv_got]).reshape(4, 4, 16, 3 * D)
    part = [part[:, s] for s in range(4)]
    part = add_up(*ring_send(part, X))
    wide = add_up(*ring_send(quarters(add_up(*wide)), X))
    part = add_up(*ring_send([part[s] for s in range(4)], "z"))
    both = ring_send(quarters(jnp.concatenate([part, wide], 1)), "y")
    shaped = grad_latent.reshape(
        row_count // WIN_LAT, col_count // WIN_LON, WIN_LAT, WIN_LON, D
    )
    grad_latent = shaped.transpose(0, 2, 1, 3, 4).reshape(row_count, col_count, D)
    grad_cols = shifted_2(grad_latent[:, col_count - half_cols :], LON, 1)
    grad_moved = jnp.concatenate([grad_cols, grad_latent[:, : col_count - half_cols]], 1)
    grad_rows = shifted_2(grad_moved[row_count - half_rows :], LAT, 1)
    grad_latent = jnp.concatenate([grad_rows, grad_moved[: row_count - half_rows]], 0)
    both = add_up(*both, True)
    return (
        grad_latent,
        both[:, : 3 * D],
        both[:, 9 * D : 10 * D],
        both[:, 5 * D : 9 * D],
        both[:, 10 * D :].reshape(4, 4, D).transpose(1, 0, 2).reshape(16, D),
        both[:, 3 * D : 5 * D],
    )


def solution(mesh):
    fine = Mesh(mesh.devices.reshape(2, 4, 2, 4, 2), LAT + LON)
    grid = P(LAT, LON)
    rows = P(LAT + LON, None)
    return jax.shard_map(
        local,
        mesh=fine,
        in_specs=(P(LAT, LON, None), P(), P(), P(), P(), P(), P(LAT, LON, None), grid),
        out_specs=(P(LAT, LON, None), rows, rows, rows, rows, rows),
        check_vma=False,
    )
```

```python
import math

import jax
import jax.numpy as jnp
from jax import lax
from jax.experimental import pallas as pl
from jax.experimental.pallas import tpu as pltpu
from jax.sharding import Mesh
from jax.sharding import PartitionSpec as P

D = 512
HEADS = 8
FF = 2048
BINS = 256
VARS = 4
WIN_LAT = 6
WIN_LON = 12
HEAD_DIM = 64
TOK = WIN_LAT * WIN_LON
WINDOWS = 12
ROWS = WINDOWS * TOK
CHUNK = 432
WIDE = 640

eps = 1e-05
smear = 0.75
masked = -1e30

LAT = ("x_lo", "z")
LON = ("x_hi", "y", "core")


def normalize(values_in):
    centre = jnp.mean(values_in, -1, keepdims=True)
    offset = values_in - centre
    inverse = lax.rsqrt(jnp.mean(offset * offset, -1, keepdims=True) + eps)
    return (offset * inverse, inverse)


def norm_back(scaled, inverse, upstream):
    return inverse * (
        upstream
        - jnp.mean(upstream, -1, keepdims=True)
        - scaled * jnp.mean(upstream * scaled, -1, keepdims=True)
    )


def gelu_parts(pre_act):
    normal_cdf = 0.5 * (1.0 + lax.erf(pre_act * (1.0 / math.sqrt(2.0))))
    density = jnp.exp(-0.5 * pre_act * pre_act) * (1.0 / math.sqrt(2.0 * math.pi))
    return (pre_act * normal_cdf, normal_cdf + pre_act * density)


def low_lanes():
    lane = lax.broadcasted_iota(jnp.int32, (1, 2 * HEAD_DIM), 1)
    return (lane < HEAD_DIM).astype(jnp.float32)


def own_lanes(stacked, low):
    return jnp.where(low > 0.5, stacked[:TOK], stacked[TOK:])


def both_heads(pair, low):
    wide = pair.astype(jnp.float32)
    return jnp.concatenate([wide * low, wide * (1.0 - low)], 0).astype(jnp.bfloat16)


def dot_nn(a, b):
    return lax.dot_general(a, b, (((1,), (0,)), ((), ())), preferred_element_type=jnp.float32)


def dot_tn(a, b):
    return lax.dot_general(a, b, (((0,), (0,)), ((), ())), preferred_element_type=jnp.float32)


def dot_nt(a, b):
    return lax.dot_general(a, b, (((1,), (1,)), ((), ())), preferred_element_type=jnp.float32)


def forward_kernel(
    at_ref, xe_ref, sort_ref, sort_tall_ref, wqkv_ref, wproj_ref, wfc1_ref, wfc2_ref, whead_ref,
    qkv_ref, probs_ref, dctx_ref, dres_ref, gown_ref, gother_ref,
    ctx32_ref, ctx_ref, n2_ref, act_ref, slope_ref, dpre_ref, n3_ref, dlog_ref, doutb_ref,
):
    def project(c, carry):
        rows = pl.ds(pl.multiple_of(c * CHUNK, CHUNK), CHUNK)
        scaled, _ = normalize(xe_ref[rows, :D].astype(jnp.float32))
        normed = scaled.astype(jnp.bfloat16)
        for j in range(3):
            part = dot_nn(normed, wqkv_ref[:, j * D : (j + 1) * D])
            for i in range(CHUNK // TOK):
                qkv_ref[c * (CHUNK // TOK) + i, :, j * D : (j + 1) * D] = part[
                    i * TOK : (i + 1) * TOK
                ].astype(jnp.bfloat16)
        return carry

    lax.fori_loop(0, ROWS // CHUNK, project, 0)

    low = low_lanes()
    q_late = lax.broadcasted_iota(jnp.int32, (2 * TOK, TOK), 0) % TOK >= TOK // 2
    k_late = lax.broadcasted_iota(jnp.int32, (2 * TOK, TOK), 1) >= TOK // 2
    apart = jnp.where(q_late == k_late, 0.0, 1.0)
    last = at_ref[3]

    def attend(w, carry):
        split = jnp.where(jnp.logical_and(last > 0, w >= WINDOWS // 2), 1.0, 0.0)
        block = apart * split
        for pair in range(HEADS // 2):
            at = pair * 2 * HEAD_DIM
            q = both_heads(qkv_ref[w, :, at : at + 128], low)
            k = qkv_ref[w, :, D + at : D + at + 128]
            v = qkv_ref[w, :, 2 * D + at : 2 * D + at + 128]
            s = dot_nt(q, k) * HEAD_DIM ** (-0.5)
            s = jnp.where(block > 0.5, masked, s)
            ex = jnp.exp(s - jnp.max(s, -1, keepdims=True))
            p = (ex / jnp.sum(ex, -1, keepdims=True)).astype(jnp.bfloat16)
            probs_ref[w, pair] = p
            ctx32_ref[pl.ds(pl.multiple_of(w * TOK, 8), TOK), at : at + 128] = own_lanes(
                dot_nn(p, v), low
            )
        return carry

    lax.fori_loop(0, WINDOWS, attend, 0)

    edge = lax.broadcasted_iota(jnp.int32, (1, BINS), 1).astype(jnp.float32)
    width = 1.0 / (smear * math.sqrt(2.0))

    def dense(c, carry):
        rows = pl.ds(pl.multiple_of(c * CHUNK, CHUNK), CHUNK)
        ctx = ctx32_ref[rows, :].astype(jnp.bfloat16)
        ctx_ref[rows, :] = dot_nt(ctx, sort_ref[...]).astype(jnp.bfloat16)
        attended = dot_nn(ctx, wproj_ref[...]).astype(jnp.bfloat16)
        residual = xe_ref[rows, :D].astype(jnp.float32) + attended.astype(jnp.float32)
        scaled2, inverse2 = normalize(residual)
        n2 = scaled2.astype(jnp.bfloat16)
        n2_ref[rows, :] = dot_nt(n2, sort_ref[...]).astype(jnp.bfloat16)
        out = residual
        for j in range(FF // D):
            cols = slice(j * D, (j + 1) * D)
            act, slope = gelu_parts(dot_nn(n2, wfc1_ref[:, cols]))
            act = act.astype(jnp.bfloat16)
            act_ref[rows, cols] = dot_nt(act, sort_tall_ref[...]).astype(jnp.bfloat16)
            slope_ref[:, cols] = slope
            out = out + dot_nn(act, wfc2_ref[cols, :])
        scaled3, inverse3 = normalize(out)
        n3 = scaled3.astype(jnp.bfloat16)
        n3_ref[rows, :] = dot_nt(n3, sort_ref[...]).astype(jnp.bfloat16)
        extra = xe_ref[rows, D : D + 128].astype(jnp.float32)
        weight = extra[:, VARS : VARS + 1] / VARS
        dz = jnp.zeros((CHUNK, D), jnp.float32)
        for v in range(VARS):
            cols = slice(v * BINS, (v + 1) * BINS)
            logits = dot_nn(n3, whead_ref[:, cols])
            ex = jnp.exp(logits - jnp.max(logits, -1, keepdims=True))
            probs = ex / jnp.sum(ex, -1, keepdims=True)
            centre = extra[:, v : v + 1] + 0.5
            mass = lax.erf((edge + 1.0 - centre) * width) - lax.erf((edge - centre) * width)
            total = lax.erf((BINS - centre) * width) - lax.erf((0.0 - centre) * width)
            d_log = (weight * (probs - mass / total)).astype(jnp.bfloat16)
            dlog_ref[rows, cols] = d_log
            dz = dz + dot_nt(d_log, whead_ref[:, cols])
        d_out = norm_back(scaled3, inverse3, dz)
        d_outb = d_out.astype(jnp.bfloat16)
        doutb_ref[rows, :] = d_outb
        dn = jnp.zeros((CHUNK, D), jnp.float32)
        for j in range(FF // D):
            cols = slice(j * D, (j + 1) * D)
            d_pre = (dot_nt(d_outb, wfc2_ref[cols, :]) * slope_ref[:, cols]).astype(jnp.bfloat16)
            dpre_ref[rows, cols] = d_pre
            dn = dn + dot_nt(d_pre, wfc1_ref[:, cols])
        d_res = d_out + norm_back(scaled2, inverse2, dn)
        dres_ref[rows, :] = d_res
        d_ctx = dot_nt(d_res.astype(jnp.bfloat16), wproj_ref[...])
        for i in range(CHUNK // TOK):
            dctx_ref[c * (CHUNK // TOK) + i] = d_ctx[i * TOK : (i + 1) * TOK].astype(jnp.bfloat16)
        return carry

    lax.fori_loop(0, ROWS // CHUNK, dense, 0)

    def keep(at, grad):
        gown_ref[:, at : at + D] = grad[: D // 2].astype(jnp.bfloat16)
        gother_ref[:, at : at + D] = grad[D // 2 :].astype(jnp.bfloat16)

    for j in range(2):
        keep(j * D, dot_tn(n3_ref[...], dlog_ref[:, j * D : (j + 1) * D]))
    for j in range(FF // D):
        cols = slice(j * D, (j + 1) * D)
        keep(2 * D + j * D, dot_tn(n2_ref[...], dpre_ref[:, cols]))
    keep(6 * D, dot_tn(ctx_ref[...], dres_ref[...].astype(jnp.bfloat16)))
    for m in range(FF // D):
        grad = dot_tn(act_ref[:, m * D : (m + 1) * D], doutb_ref[...]).astype(jnp.bfloat16)
        for t in range(32):
            i1, core, z_low, x_hi = (t // 8, t // 4 % 2, t // 2 % 2, t % 2)
            z = (m % 2 * 2 + z_low + 4 - at_ref[2]) % 4
            x = (x_hi * 2 + m // 2 + 4 - at_ref[0]) % 4
            rows = pl.ds(pl.multiple_of(z * 64 + x * 16, 16), 16)
            target = gother_ref if core else gown_ref
            target[rows, 7 * D + i1 * D : 8 * D + i1 * D] = grad[t * 16 : (t + 1) * 16]


def attention_back_kernel(
    qkv_ref, probs_ref, dctx_ref, dqkv_ref, dqkv32_ref
):
    low = low_lanes()

    def attend(w, carry):
        rows = pl.ds(pl.multiple_of(w * TOK, 8), TOK)
        for pair in range(HEADS // 2):
            at = pair * 2 * HEAD_DIM
            q = both_heads(qkv_ref[w, :, at : at + 128], low)
            k = qkv_ref[w, :, D + at : D + at + 128]
            v = qkv_ref[w, :, 2 * D + at : 2 * D + at + 128]
            up = both_heads(dctx_ref[w, :, at : at + 128], low)
            p = probs_ref[w, pair]
            p32 = p.astype(jnp.float32)
            d_p = dot_nt(up, v)
            d_s = p32 * (d_p - jnp.sum(d_p * p32, -1, keepdims=True)) * HEAD_DIM ** (-0.5)
            d_s = d_s.astype(jnp.bfloat16)
            dqkv32_ref[rows, at : at + 128] = own_lanes(dot_nn(d_s, k), low)
            dqkv32_ref[rows, D + at : D + at + 128] = dot_tn(d_s, q)
            dqkv32_ref[rows, 2 * D + at : 2 * D + at + 128] = dot_tn(p, up)
        return carry

    lax.fori_loop(0, WINDOWS // 2, attend, 0)
    dqkv_ref[...] = dqkv32_ref[...].astype(jnp.bfloat16)


def finish_kernel(
    xe_ref, sort_ref, dqkv_a_ref, dqkv_b_ref, dres_ref, wqkv_ref,
    glat_ref, gown_ref, gother_ref,
    n1_ref,
):
    half = ROWS // 2
    for c, dqkv_ref in enumerate((dqkv_a_ref, dqkv_b_ref)):
        rows = slice(c * half, (c + 1) * half)
        scaled1, inverse1 = normalize(xe_ref[rows, :D].astype(jnp.float32))
        n1_ref[c] = dot_nt(scaled1.astype(jnp.bfloat16), sort_ref[...]).astype(jnp.bfloat16)
        d_sh = dot_nt(dqkv_ref[...], wqkv_ref[...]).astype(jnp.bfloat16).astype(jnp.float32)
        glat_ref[rows, :] = (dres_ref[rows, :] + norm_back(scaled1, inverse1, d_sh)).astype(
            jnp.bfloat16
        )
    for j in range(3):
        cols = slice(j * D, (j + 1) * D)
        grad = dot_tn(n1_ref[0], dqkv_a_ref[:, cols]) + dot_tn(n1_ref[1], dqkv_b_ref[:, cols])
        gown_ref[:, cols] = grad[: D // 2].astype(jnp.bfloat16)
        gother_ref[:, cols] = grad[D // 2 :].astype(jnp.bfloat16)


def whole(shape, dtype):
    return jax.ShapeDtypeStruct(shape, dtype)


VMEM_SPEC = pl.BlockSpec(memory_space=pltpu.VMEM)


def run_forward(at, xe, sort, sort_tall, w_qkv, w_proj, w_fc1, w_fc2, w_head):
    bf, f32 = (jnp.bfloat16, jnp.float32)
    return pl.pallas_call(
        forward_kernel,
        out_shape=(
            whole((WINDOWS, TOK, 3 * D), bf),
            whole((WINDOWS, HEADS // 2, 2 * TOK, TOK), bf),
            whole((WINDOWS, TOK, D), bf),
            whole((ROWS, D), f32),
            whole((D // 2, 11 * D), bf),
            whole((D // 2, 11 * D), bf),
        ),
        in_specs=[pl.BlockSpec(memory_space=pltpu.SMEM)] + [VMEM_SPEC] * 8,
        out_specs=(VMEM_SPEC,) * 6,
        scratch_shapes=[
            pltpu.VMEM((ROWS, D), f32),
            pltpu.VMEM((ROWS, D), bf),
            pltpu.VMEM((ROWS, D), bf),
            pltpu.VMEM((ROWS, FF), bf),
            pltpu.VMEM((CHUNK, FF), f32),
            pltpu.VMEM((ROWS, FF), bf),
            pltpu.VMEM((ROWS, D), bf),
            pltpu.VMEM((ROWS, VARS * BINS), bf),
            pltpu.VMEM((ROWS, D), bf),
        ],
        compiler_params=pltpu.CompilerParams(vmem_limit_bytes=60 * 1024 * 1024),
        name="forward",
    )(at, xe, sort, sort_tall, w_qkv, w_proj, w_fc1, w_fc2, w_head)


def run_attention_back(part, qkv, probs, d_ctx):
    bf, f32 = (jnp.bfloat16, jnp.float32)
    half = WINDOWS // 2
    return pl.pallas_call(
        attention_back_kernel,
        out_shape=whole((ROWS // 2, 3 * D), bf),
        grid=(1,),
        in_specs=[
            pl.BlockSpec((half, TOK, 3 * D), lambda i: (part, 0, 0)),
            pl.BlockSpec((half, HEADS // 2, 2 * TOK, TOK), lambda i: (part, 0, 0, 0)),
            pl.BlockSpec((half, TOK, D), lambda i: (part, 0, 0)),
        ],
        out_specs=pl.BlockSpec((ROWS // 2, 3 * D), lambda i: (0, 0)),
        scratch_shapes=[pltpu.VMEM((ROWS // 2, 3 * D), f32)],
        compiler_params=pltpu.CompilerParams(vmem_limit_bytes=48 * 1024 * 1024),
        name="attention_back",
        cost_estimate=pl.CostEstimate(
            flops=10**9, transcendentals=0, bytes_accessed=4 * 10**6
        ),
    )(qkv, probs, d_ctx)


def run_finish(xe, sort, dqkv_a, dqkv_b, d_res, w_qkv):
    bf = jnp.bfloat16
    return pl.pallas_call(
        finish_kernel,
        out_shape=(
            whole((ROWS, D), bf),
            whole((D // 2, 3 * D), bf),
            whole((D // 2, 3 * D), bf),
        ),
        in_specs=[VMEM_SPEC] * 6,
        out_specs=(VMEM_SPEC,) * 3,
        scratch_shapes=[pltpu.VMEM((2, ROWS // 2, D), bf)],
        compiler_params=pltpu.CompilerParams(vmem_limit_bytes=48 * 1024 * 1024),
        name="finish",
        cost_estimate=pl.CostEstimate(
            flops=10**9, transcendentals=0, bytes_accessed=8 * 10**6
        ),
    )(xe, sort, dqkv_a, dqkv_b, d_res, w_qkv)


def place():
    x = lax.axis_index("x_hi") * 2 + lax.axis_index("x_lo")
    return (x, lax.axis_index("y"), lax.axis_index("z"), lax.axis_index("core"))


def sorter():
    x_me, y_me, z_me, core_me = place()
    at = lax.broadcasted_iota(jnp.int32, (D, 1), 0)
    source = lax.broadcasted_iota(jnp.int32, (D, D), 1)
    core = (at // 256 + core_me) % 2
    z = (at // 64 + z_me) % 4
    x = (at // 16 + x_me) % 4
    y = (at // 4 + y_me) % 4
    owner = ((((x % 2) * 4 + z) * 2 + x // 2) * 4 + y) * 2 + core
    return (source == owner * 4 + at % 4).astype(jnp.bfloat16)


def tall_sorter():
    _, y_me, _, core_me = place()
    at = lax.broadcasted_iota(jnp.int32, (D, 1), 0)
    source = lax.broadcasted_iota(jnp.int32, (D, D), 1)
    core = (at // 64 + core_me) % 2
    y = (at // 4 + y_me) % 4
    owner = (at // 16 % 4 * 4 + y) * 2 + core
    return (source == owner * 16 + at // 128 * 4 + at % 4).astype(jnp.bfloat16)


def ring_pairs(axes, step):
    if isinstance(axes, str):
        return [(i, (i + step) % 4) for i in range(4)]
    spot = [(i % 2) * 2 + i // 2 for i in range(4)]
    return [(spot[i], spot[(i + step) % 4]) for i in range(4)]


X = ("x_lo", "x_hi")


def add_up(own, arrived, last=False):
    total = own.astype(jnp.float32)
    for part in arrived:
        total = total + part.astype(jnp.float32)
    return total if last else total.astype(jnp.bfloat16)


def ring_send(blocks, axes):
    return (
        blocks[0],
        [lax.ppermute(blocks[s], axes, ring_pairs(axes, s)) for s in (2, 1, 3)],
    )


def quarters(value):
    n = value.shape[0] // 4
    return [value[i * n : (i + 1) * n] for i in range(4)]


def core_send(value):
    return lax.ppermute(value, "core", [(0, 1), (1, 0)])


def shifted_2(value, axis, steps):
    count = lax.axis_size(axis)
    pairs = [(source, (source + steps) % count) for source in range(count)]
    return lax.ppermute(value, axis, pairs)


def local(latent, w_qkv, w_proj, w_fc1, w_fc2, w_head, target_bins, land_mask):
    row_count, col_count, _ = latent.shape
    half_rows = WIN_LAT // 2
    half_cols = WIN_LON // 2
    bf = jnp.bfloat16
    ext = jnp.concatenate(
        [
            latent,
            target_bins.astype(bf),
            land_mask[:, :, None].astype(bf),
            jnp.zeros((row_count, col_count, WIDE - D - VARS - 1), bf),
        ],
        2,
    )
    edge_cols = shifted_2(ext[:, :half_cols], LON, -1)
    moved = jnp.concatenate([ext[:, half_cols:], edge_cols], 1)
    edge_rows = shifted_2(moved[:half_rows], LAT, -1)
    block = jnp.concatenate([moved[half_rows:], edge_rows], 0)
    shaped = block.reshape(row_count // WIN_LAT, WIN_LAT, col_count // WIN_LON, WIN_LON, WIDE)
    xe = shaped.transpose(0, 2, 1, 3, 4).reshape(ROWS, WIDE)
    last = (lax.axis_index(LAT) == lax.axis_size(LAT) - 1).astype(jnp.int32)
    x_me, y_me, z_me, _ = place()
    at = jnp.stack([x_me, y_me, z_me, last])
    sort = sorter()
    qkv, probs, d_ctx, d_res, wide_own, wide_other = run_forward(
        at, xe, sort, tall_sorter(), w_qkv, w_proj, w_fc1, w_fc2, w_head
    )
    wide_got = core_send(wide_other)
    d_qkv_a = run_attention_back(0, qkv, probs, d_ctx)
    wide = ring_send(quarters(add_up(wide_own, [wide_got])), "z")
    d_qkv_b = run_attention_back(1, qkv, probs, d_ctx)
    grad_latent, qkv_own, qkv_other = run_finish(xe, sort, d_qkv_a, d_qkv_b, d_res, w_qkv)
    qkv_got = core_send(qkv_other)
    part = add_up(qkv_own, [qkv_got]).reshape(4, 4, 16, 3 * D)
    part = [part[:, s] for s in range(4)]
    part = add_up(*ring_send(part, X))
    wide = add_up(*ring_send(quarters(add_up(*wide)), X))
    part = add_up(*ring_send([part[s] for s in range(4)], "z"))
    both = ring_send(quarters(jnp.concatenate([part, wide], 1)), "y")
    shaped = grad_latent.reshape(
        row_count // WIN_LAT, col_count // WIN_LON, WIN_LAT, WIN_LON, D
    )
    grad_latent = shaped.transpose(0, 2, 1, 3, 4).reshape(row_count, col_count, D)
    grad_cols = shifted_2(grad_latent[:, col_count - half_cols :], LON, 1)
    grad_moved = jnp.concatenate([grad_cols, grad_latent[:, : col_count - half_cols]], 1)
    grad_rows = shifted_2(grad_moved[row_count - half_rows :], LAT, 1)
    grad_latent = jnp.concatenate([grad_rows, grad_moved[: row_count - half_rows]], 0)
    both = add_up(*both, True)
    return (
        grad_latent,
        both[:, : 3 * D],
        both[:, 9 * D : 10 * D],
        both[:, 5 * D : 9 * D],
        both[:, 10 * D :].reshape(4, 4, D).transpose(1, 0, 2).reshape(16, D),
        both[:, 3 * D : 5 * D],
    )


def solution(mesh):
    fine = Mesh(mesh.devices.reshape(2, 4, 2, 4, 2), LAT + LON)
    grid = P(LAT, LON)
    rows = P(LAT + LON, None)
    return jax.shard_map(
        local,
        mesh=fine,
        in_specs=(P(LAT, LON, None), P(), P(), P(), P(), P(), P(LAT, LON, None), grid),
        out_specs=(P(LAT, LON, None), rows, rows, rows, rows, rows),
        check_vma=False,
    )
```

```python
import math

import jax
import jax.numpy as jnp
from jax import lax
from jax.experimental import pallas as pl
from jax.experimental.pallas import tpu as pltpu
from jax.sharding import Mesh
from jax.sharding import PartitionSpec as P

D = 512
HEADS = 8
FF = 2048
BINS = 256
VARS = 4
WIN_LAT = 6
WIN_LON = 12
HEAD_DIM = 64
TOK = WIN_LAT * WIN_LON
WINDOWS = 12
ROWS = WINDOWS * TOK
CHUNK = 432
WIDE = 640
NROWS = 12
NCOLS = 72
HALF_ROWS = WIN_LAT // 2
HALF_COLS = WIN_LON // 2

eps = 1e-05
smear = 0.75
masked = -1e30

LAT = ("x_lo", "z")
LON = ("x_hi", "y", "core")


def normalize(values_in):
    centre = jnp.mean(values_in, -1, keepdims=True)
    offset = values_in - centre
    inverse = lax.rsqrt(jnp.mean(offset * offset, -1, keepdims=True) + eps)
    return (offset * inverse, inverse)


def norm_back(scaled, inverse, upstream):
    return inverse * (
        upstream
        - jnp.mean(upstream, -1, keepdims=True)
        - scaled * jnp.mean(upstream * scaled, -1, keepdims=True)
    )


def gelu_parts(pre_act):
    normal_cdf = 0.5 * (1.0 + lax.erf(pre_act * (1.0 / math.sqrt(2.0))))
    density = jnp.exp(-0.5 * pre_act * pre_act) * (1.0 / math.sqrt(2.0 * math.pi))
    return (pre_act * normal_cdf, normal_cdf + pre_act * density)


def window_row(r, c):
    return ((r // WIN_LAT) * (NCOLS // WIN_LON) + c) * TOK + r % WIN_LAT * WIN_LON


def low_lanes():
    lane = lax.broadcasted_iota(jnp.int32, (1, 2 * HEAD_DIM), 1)
    return (lane < HEAD_DIM).astype(jnp.float32)


def own_lanes(stacked, low):
    return jnp.where(low > 0.5, stacked[:TOK], stacked[TOK:])


def both_heads(pair, low):
    wide = pair.astype(jnp.float32)
    return jnp.concatenate([wide * low, wide * (1.0 - low)], 0).astype(jnp.bfloat16)


def dot_nn(a, b):
    return lax.dot_general(a, b, (((1,), (0,)), ((), ())), preferred_element_type=jnp.float32)


def dot_tn(a, b):
    return lax.dot_general(a, b, (((0,), (0,)), ((), ())), preferred_element_type=jnp.float32)


def dot_nt(a, b):
    return lax.dot_general(a, b, (((1,), (1,)), ((), ())), preferred_element_type=jnp.float32)


def forward_kernel(
    at_ref, main_ref, aux_ref, col_ref, row_ref, corner_ref,
    sort_ref, sort_tall_ref, wqkv_ref, wproj_ref, wfc1_ref, wfc2_ref, whead_ref,
    xw_ref, qkv_ref, probs_ref, dctx_ref, dres_ref, gown_ref, gother_ref,
    ctx32_ref, ctx_ref, n2_ref, act_ref, slope_ref, dpre_ref, n3_ref, dlog_ref, doutb_ref,
    x32_ref, lines_ref,
):
    for r in range(NROWS):
        if r < NROWS - HALF_ROWS:
            lines_ref[r, :NCOLS, :D] = main_ref[r + HALF_ROWS].astype(jnp.float32)
            lines_ref[r, :NCOLS, D:] = aux_ref[r + HALF_ROWS].astype(jnp.float32)
            lines_ref[r, NCOLS : NCOLS + HALF_COLS, :] = col_ref[r].astype(jnp.float32)
        else:
            far = r + HALF_ROWS - NROWS
            lines_ref[r, :NCOLS, :] = row_ref[far].astype(jnp.float32)
            lines_ref[r, NCOLS : NCOLS + HALF_COLS, :] = corner_ref[far].astype(jnp.float32)
        for c in range(NCOLS // WIN_LON):
            first = window_row(r, c)
            x32_ref[first : first + WIN_LON, :] = lines_ref[
                r, c * WIN_LON + HALF_COLS : (c + 1) * WIN_LON + HALF_COLS, :
            ]
    xw_ref[...] = x32_ref[:, :D].astype(jnp.bfloat16)

    def project(c, carry):
        rows = pl.ds(pl.multiple_of(c * CHUNK, CHUNK), CHUNK)
        scaled, _ = normalize(x32_ref[rows, :D])
        normed = scaled.astype(jnp.bfloat16)
        for j in range(3):
            part = dot_nn(normed, wqkv_ref[:, j * D : (j + 1) * D])
            for i in range(CHUNK // TOK):
                qkv_ref[c * (CHUNK // TOK) + i, :, j * D : (j + 1) * D] = part[
                    i * TOK : (i + 1) * TOK
                ].astype(jnp.bfloat16)
        return carry

    lax.fori_loop(0, ROWS // CHUNK, project, 0)

    low = low_lanes()
    q_late = lax.broadcasted_iota(jnp.int32, (2 * TOK, TOK), 0) % TOK >= TOK // 2
    k_late = lax.broadcasted_iota(jnp.int32, (2 * TOK, TOK), 1) >= TOK // 2
    apart = jnp.where(q_late == k_late, 0.0, 1.0)
    last = at_ref[3]

    def attend(w, carry):
        split = jnp.where(jnp.logical_and(last > 0, w >= WINDOWS // 2), 1.0, 0.0)
        block = apart * split
        for pair in range(HEADS // 2):
            at = pair * 2 * HEAD_DIM
            q = both_heads(qkv_ref[w, :, at : at + 128], low)
            k = qkv_ref[w, :, D + at : D + at + 128]
            v = qkv_ref[w, :, 2 * D + at : 2 * D + at + 128]
            s = dot_nt(q, k) * HEAD_DIM ** (-0.5)
            s = jnp.where(block > 0.5, masked, s)
            ex = jnp.exp(s - jnp.max(s, -1, keepdims=True))
            p = (ex / jnp.sum(ex, -1, keepdims=True)).astype(jnp.bfloat16)
            probs_ref[w, pair] = p
            ctx32_ref[pl.ds(pl.multiple_of(w * TOK, 8), TOK), at : at + 128] = own_lanes(
                dot_nn(p, v), low
            )
        return carry

    lax.fori_loop(0, WINDOWS, attend, 0)

    edge = lax.broadcasted_iota(jnp.int32, (1, BINS), 1).astype(jnp.float32)
    width = 1.0 / (smear * math.sqrt(2.0))

    def dense(c, carry):
        rows = pl.ds(pl.multiple_of(c * CHUNK, CHUNK), CHUNK)
        ctx = ctx32_ref[rows, :].astype(jnp.bfloat16)
        ctx_ref[rows, :] = dot_nt(ctx, sort_ref[...]).astype(jnp.bfloat16)
        attended = dot_nn(ctx, wproj_ref[...]).astype(jnp.bfloat16)
        residual = x32_ref[rows, :D] + attended.astype(jnp.float32)
        scaled2, inverse2 = normalize(residual)
        n2 = scaled2.astype(jnp.bfloat16)
        n2_ref[rows, :] = dot_nt(n2, sort_ref[...]).astype(jnp.bfloat16)
        out = residual
        for j in range(FF // D):
            cols = slice(j * D, (j + 1) * D)
            act, slope = gelu_parts(dot_nn(n2, wfc1_ref[:, cols]))
            act = act.astype(jnp.bfloat16)
            act_ref[rows, cols] = dot_nt(act, sort_tall_ref[...]).astype(jnp.bfloat16)
            slope_ref[:, cols] = slope
            out = out + dot_nn(act, wfc2_ref[cols, :])
        scaled3, inverse3 = normalize(out)
        n3 = scaled3.astype(jnp.bfloat16)
        n3_ref[rows, :] = dot_nt(n3, sort_ref[...]).astype(jnp.bfloat16)
        extra = x32_ref[rows, D : D + 128]
        weight = extra[:, VARS : VARS + 1] / VARS
        dz = jnp.zeros((CHUNK, D), jnp.float32)
        for v in range(VARS):
            cols = slice(v * BINS, (v + 1) * BINS)
            logits = dot_nn(n3, whead_ref[:, cols])
            ex = jnp.exp(logits - jnp.max(logits, -1, keepdims=True))
            probs = ex / jnp.sum(ex, -1, keepdims=True)
            centre = extra[:, v : v + 1] + 0.5
            mass = lax.erf((edge + 1.0 - centre) * width) - lax.erf((edge - centre) * width)
            total = lax.erf((BINS - centre) * width) - lax.erf((0.0 - centre) * width)
            d_log = (weight * (probs - mass / total)).astype(jnp.bfloat16)
            dlog_ref[rows, cols] = d_log
            dz = dz + dot_nt(d_log, whead_ref[:, cols])
        d_out = norm_back(scaled3, inverse3, dz)
        d_outb = d_out.astype(jnp.bfloat16)
        doutb_ref[rows, :] = d_outb
        dn = jnp.zeros((CHUNK, D), jnp.float32)
        for j in range(FF // D):
            cols = slice(j * D, (j + 1) * D)
            d_pre = (dot_nt(d_outb, wfc2_ref[cols, :]) * slope_ref[:, cols]).astype(jnp.bfloat16)
            dpre_ref[rows, cols] = d_pre
            dn = dn + dot_nt(d_pre, wfc1_ref[:, cols])
        d_res = d_out + norm_back(scaled2, inverse2, dn)
        dres_ref[rows, :] = d_res
        d_ctx = dot_nt(d_res.astype(jnp.bfloat16), wproj_ref[...])
        for i in range(CHUNK // TOK):
            dctx_ref[c * (CHUNK // TOK) + i] = d_ctx[i * TOK : (i + 1) * TOK].astype(jnp.bfloat16)
        return carry

    lax.fori_loop(0, ROWS // CHUNK, dense, 0)

    def keep(at, grad):
        gown_ref[:, at : at + D] = grad[: D // 2].astype(jnp.bfloat16)
        gother_ref[:, at : at + D] = grad[D // 2 :].astype(jnp.bfloat16)

    for j in range(2):
        keep(j * D, dot_tn(n3_ref[...], dlog_ref[:, j * D : (j + 1) * D]))
    for j in range(FF // D):
        cols = slice(j * D, (j + 1) * D)
        keep(2 * D + j * D, dot_tn(n2_ref[...], dpre_ref[:, cols]))
    keep(6 * D, dot_tn(ctx_ref[...], dres_ref[...].astype(jnp.bfloat16)))
    for m in range(FF // D):
        grad = dot_tn(act_ref[:, m * D : (m + 1) * D], doutb_ref[...]).astype(jnp.bfloat16)
        for t in range(32):
            i1, core, z_low, x_hi = (t // 8, t // 4 % 2, t // 2 % 2, t % 2)
            z = (m % 2 * 2 + z_low + 4 - at_ref[2]) % 4
            x = (x_hi * 2 + m // 2 + 4 - at_ref[0]) % 4
            rows = pl.ds(pl.multiple_of(z * 64 + x * 16, 16), 16)
            target = gother_ref if core else gown_ref
            target[rows, 7 * D + i1 * D : 8 * D + i1 * D] = grad[t * 16 : (t + 1) * 16]


def attention_back_kernel(
    qkv_ref, probs_ref, dctx_ref, dqkv_ref, dqkv32_ref
):
    low = low_lanes()

    def attend(w, carry):
        rows = pl.ds(pl.multiple_of(w * TOK, 8), TOK)
        for pair in range(HEADS // 2):
            at = pair * 2 * HEAD_DIM
            q = both_heads(qkv_ref[w, :, at : at + 128], low)
            k = qkv_ref[w, :, D + at : D + at + 128]
            v = qkv_ref[w, :, 2 * D + at : 2 * D + at + 128]
            up = both_heads(dctx_ref[w, :, at : at + 128], low)
            p = probs_ref[w, pair]
            p32 = p.astype(jnp.float32)
            d_p = dot_nt(up, v)
            d_s = p32 * (d_p - jnp.sum(d_p * p32, -1, keepdims=True)) * HEAD_DIM ** (-0.5)
            d_s = d_s.astype(jnp.bfloat16)
            dqkv32_ref[rows, at : at + 128] = own_lanes(dot_nn(d_s, k), low)
            dqkv32_ref[rows, D + at : D + at + 128] = dot_tn(d_s, q)
            dqkv32_ref[rows, 2 * D + at : 2 * D + at + 128] = dot_tn(p, up)
        return carry

    lax.fori_loop(0, WINDOWS // 2, attend, 0)
    dqkv_ref[...] = dqkv32_ref[...].astype(jnp.bfloat16)


def finish_kernel(
    xw_ref, sort_ref, dqkv_a_ref, dqkv_b_ref, dres_ref, wqkv_ref,
    glat_ref, gown_ref, gother_ref,
    n1_ref, glat32_ref, line_ref,
):
    half = ROWS // 2
    for c, dqkv_ref in enumerate((dqkv_a_ref, dqkv_b_ref)):
        rows = slice(c * half, (c + 1) * half)
        scaled1, inverse1 = normalize(xw_ref[rows, :].astype(jnp.float32))
        n1_ref[c] = dot_nt(scaled1.astype(jnp.bfloat16), sort_ref[...]).astype(jnp.bfloat16)
        d_sh = dot_nt(dqkv_ref[...], wqkv_ref[...]).astype(jnp.bfloat16).astype(jnp.float32)
        glat32_ref[rows, :] = dres_ref[rows, :] + norm_back(scaled1, inverse1, d_sh)
    for r in range(NROWS):
        for c in range(NCOLS // WIN_LON):
            first = window_row(r, c)
            line_ref[r, c * WIN_LON : (c + 1) * WIN_LON, :] = glat32_ref[
                first : first + WIN_LON, :
            ]
        glat_ref[r] = line_ref[r].astype(jnp.bfloat16)
    for j in range(3):
        cols = slice(j * D, (j + 1) * D)
        grad = dot_tn(n1_ref[0], dqkv_a_ref[:, cols]) + dot_tn(n1_ref[1], dqkv_b_ref[:, cols])
        gown_ref[:, cols] = grad[: D // 2].astype(jnp.bfloat16)
        gother_ref[:, cols] = grad[D // 2 :].astype(jnp.bfloat16)


def whole(shape, dtype):
    return jax.ShapeDtypeStruct(shape, dtype)


VMEM_SPEC = pl.BlockSpec(memory_space=pltpu.VMEM)


def run_forward(at, blocks, sort, sort_tall, w_qkv, w_proj, w_fc1, w_fc2, w_head):
    bf, f32 = (jnp.bfloat16, jnp.float32)
    return pl.pallas_call(
        forward_kernel,
        out_shape=(
            whole((ROWS, D), bf),
            whole((WINDOWS, TOK, 3 * D), bf),
            whole((WINDOWS, HEADS // 2, 2 * TOK, TOK), bf),
            whole((WINDOWS, TOK, D), bf),
            whole((ROWS, D), f32),
            whole((D // 2, 11 * D), bf),
            whole((D // 2, 11 * D), bf),
        ),
        in_specs=[pl.BlockSpec(memory_space=pltpu.SMEM)] + [VMEM_SPEC] * 12,
        out_specs=(VMEM_SPEC,) * 7,
        scratch_shapes=[
            pltpu.VMEM((ROWS, D), f32),
            pltpu.VMEM((ROWS, D), bf),
            pltpu.VMEM((ROWS, D), bf),
            pltpu.VMEM((ROWS, FF), bf),
            pltpu.VMEM((CHUNK, FF), f32),
            pltpu.VMEM((ROWS, FF), bf),
            pltpu.VMEM((ROWS, D), bf),
            pltpu.VMEM((ROWS, VARS * BINS), bf),
            pltpu.VMEM((ROWS, D), bf),
            pltpu.VMEM((ROWS, WIDE), f32),
            pltpu.VMEM((NROWS, 80, WIDE), f32),
        ],
        compiler_params=pltpu.CompilerParams(vmem_limit_bytes=60 * 1024 * 1024),
        name="forward",
    )(at, *blocks, sort, sort_tall, w_qkv, w_proj, w_fc1, w_fc2, w_head)


def run_attention_back(part, qkv, probs, d_ctx):
    bf, f32 = (jnp.bfloat16, jnp.float32)
    half = WINDOWS // 2
    return pl.pallas_call(
        attention_back_kernel,
        out_shape=whole((ROWS // 2, 3 * D), bf),
        grid=(1,),
        in_specs=[
            pl.BlockSpec((half, TOK, 3 * D), lambda i: (part, 0, 0)),
            pl.BlockSpec((half, HEADS // 2, 2 * TOK, TOK), lambda i: (part, 0, 0, 0)),
            pl.BlockSpec((half, TOK, D), lambda i: (part, 0, 0)),
        ],
        out_specs=pl.BlockSpec((ROWS // 2, 3 * D), lambda i: (0, 0)),
        scratch_shapes=[pltpu.VMEM((ROWS // 2, 3 * D), f32)],
        compiler_params=pltpu.CompilerParams(vmem_limit_bytes=48 * 1024 * 1024),
        name="attention_back",
        cost_estimate=pl.CostEstimate(
            flops=10**9, transcendentals=0, bytes_accessed=4 * 10**6
        ),
    )(qkv, probs, d_ctx)


def run_finish(xw, sort, dqkv_a, dqkv_b, d_res, w_qkv):
    bf = jnp.bfloat16
    return pl.pallas_call(
        finish_kernel,
        out_shape=(
            whole((NROWS, NCOLS, D), bf),
            whole((D // 2, 3 * D), bf),
            whole((D // 2, 3 * D), bf),
        ),
        in_specs=[VMEM_SPEC] * 6,
        out_specs=(VMEM_SPEC,) * 3,
        scratch_shapes=[
            pltpu.VMEM((2, ROWS // 2, D), bf),
            pltpu.VMEM((ROWS, D), jnp.float32),
            pltpu.VMEM((NROWS, NCOLS, D), jnp.float32),
        ],
        compiler_params=pltpu.CompilerParams(vmem_limit_bytes=48 * 1024 * 1024),
        name="finish",
        cost_estimate=pl.CostEstimate(
            flops=10**9, transcendentals=0, bytes_accessed=8 * 10**6
        ),
    )(xw, sort, dqkv_a, dqkv_b, d_res, w_qkv)


def place():
    x = lax.axis_index("x_hi") * 2 + lax.axis_index("x_lo")
    return (x, lax.axis_index("y"), lax.axis_index("z"), lax.axis_index("core"))


def sorter():
    x_me, y_me, z_me, core_me = place()
    at = lax.broadcasted_iota(jnp.int32, (D, 1), 0)
    source = lax.broadcasted_iota(jnp.int32, (D, D), 1)
    core = (at // 256 + core_me) % 2
    z = (at // 64 + z_me) % 4
    x = (at // 16 + x_me) % 4
    y = (at // 4 + y_me) % 4
    owner = ((((x % 2) * 4 + z) * 2 + x // 2) * 4 + y) * 2 + core
    return (source == owner * 4 + at % 4).astype(jnp.bfloat16)


def tall_sorter():
    _, y_me, _, core_me = place()
    at = lax.broadcasted_iota(jnp.int32, (D, 1), 0)
    source = lax.broadcasted_iota(jnp.int32, (D, D), 1)
    core = (at // 64 + core_me) % 2
    y = (at // 4 + y_me) % 4
    owner = (at // 16 % 4 * 4 + y) * 2 + core
    return (source == owner * 16 + at // 128 * 4 + at % 4).astype(jnp.bfloat16)


def ring_pairs(axes, step):
    if isinstance(axes, str):
        return [(i, (i + step) % 4) for i in range(4)]
    spot = [(i % 2) * 2 + i // 2 for i in range(4)]
    return [(spot[i], spot[(i + step) % 4]) for i in range(4)]


X = ("x_lo", "x_hi")


def add_up(own, arrived, last=False):
    total = own.astype(jnp.float32)
    for part in arrived:
        total = total + part.astype(jnp.float32)
    return total if last else total.astype(jnp.bfloat16)


def ring_send(blocks, axes):
    return (
        blocks[0],
        [lax.ppermute(blocks[s], axes, ring_pairs(axes, s)) for s in (2, 1, 3)],
    )


def quarters(value):
    n = value.shape[0] // 4
    return [value[i * n : (i + 1) * n] for i in range(4)]


def core_send(value):
    return lax.ppermute(value, "core", [(0, 1), (1, 0)])


def shifted_2(value, axis, steps):
    count = lax.axis_size(axis)
    pairs = [(source, (source + steps) % count) for source in range(count)]
    return lax.ppermute(value, axis, pairs)


def diagonal(value, steps):
    rows, cols = (lax.axis_size(LAT), lax.axis_size(LON))
    pairs = [
        (r * cols + c, (r + steps) % rows * cols + (c + steps) % cols)
        for r in range(rows)
        for c in range(cols)
    ]
    return lax.ppermute(value, LAT + LON, pairs)


def local(latent, w_qkv, w_proj, w_fc1, w_fc2, w_head, target_bins, land_mask):
    bf = jnp.bfloat16

    aux = jnp.concatenate([target_bins, land_mask[:, :, None]], 2).astype(bf)
    aux = lax.optimization_barrier(jnp.pad(aux, ((0, 0), (0, 0), (0, WIDE - D - VARS - 1))))

    def edge(rows, cols):
        return jnp.concatenate([latent[rows, cols], aux[rows, cols]], 2)

    every, top, rest, left = (slice(None), slice(0, 3), slice(3, None), slice(0, 6))
    col_edge = shifted_2(edge(rest, left), LON, -1)
    row_edge = shifted_2(edge(top, every), LAT, -1)
    corner = diagonal(edge(top, left), -1)
    blocks = (latent, aux, col_edge, row_edge, corner)
    last = (lax.axis_index(LAT) == lax.axis_size(LAT) - 1).astype(jnp.int32)
    x_me, y_me, z_me, _ = place()
    at = jnp.stack([x_me, y_me, z_me, last])
    sort = sorter()
    xw, qkv, probs, d_ctx, d_res, wide_own, wide_other = run_forward(
        at, blocks, sort, tall_sorter(), w_qkv, w_proj, w_fc1, w_fc2, w_head
    )
    wide_got = core_send(wide_other)
    d_qkv_a = run_attention_back(0, qkv, probs, d_ctx)
    wide = ring_send(quarters(add_up(wide_own, [wide_got])), "z")
    d_qkv_b = run_attention_back(1, qkv, probs, d_ctx)
    grad_latent, qkv_own, qkv_other = run_finish(xw, sort, d_qkv_a, d_qkv_b, d_res, w_qkv)
    qkv_got = core_send(qkv_other)
    part = add_up(qkv_own, [qkv_got]).reshape(4, 4, 16, 3 * D)
    part = [part[:, s] for s in range(4)]
    part = add_up(*ring_send(part, X))
    wide = add_up(*ring_send(quarters(add_up(*wide)), X))
    part = add_up(*ring_send([part[s] for s in range(4)], "z"))
    both = ring_send(quarters(jnp.concatenate([part, wide], 1)), "y")
    keep_rows, keep_cols = (NROWS - HALF_ROWS, NCOLS - HALF_COLS)
    grad_cols = shifted_2(grad_latent[:keep_rows, keep_cols:], LON, 1)
    grad_rows = shifted_2(grad_latent[keep_rows:, :keep_cols], LAT, 1)
    grad_corner = diagonal(grad_latent[keep_rows:, keep_cols:], 1)
    grad_latent = jnp.concatenate(
        [
            jnp.concatenate([grad_corner, grad_rows], 1),
            jnp.concatenate([grad_cols, grad_latent[:keep_rows, :keep_cols]], 1),
        ],
        0,
    )
    both = add_up(*both, True)
    return (
        grad_latent,
        both[:, : 3 * D],
        both[:, 9 * D : 10 * D],
        both[:, 5 * D : 9 * D],
        both[:, 10 * D :].reshape(4, 4, D).transpose(1, 0, 2).reshape(16, D),
        both[:, 3 * D : 5 * D],
    )


def solution(mesh):
    fine = Mesh(mesh.devices.reshape(2, 4, 2, 4, 2), LAT + LON)
    grid = P(LAT, LON)
    rows = P(LAT + LON, None)
    return jax.shard_map(
        local,
        mesh=fine,
        in_specs=(P(LAT, LON, None), P(), P(), P(), P(), P(), P(LAT, LON, None), grid),
        out_specs=(P(LAT, LON, None), rows, rows, rows, rows, rows),
        check_vma=False,
    )
```

```python
import math

import jax
import jax.numpy as jnp
from jax import lax
from jax.experimental import pallas as pl
from jax.experimental.pallas import tpu as pltpu
from jax.sharding import Mesh
from jax.sharding import PartitionSpec as P

D = 512
HEADS = 8
FF = 2048
BINS = 256
VARS = 4
WIN_LAT = 6
WIN_LON = 12
HEAD_DIM = 64
TOK = WIN_LAT * WIN_LON
WINDOWS = 12
ROWS = WINDOWS * TOK
CHUNK = 432
WIDE = 640
NROWS = 12
NCOLS = 72
HALF_ROWS = WIN_LAT // 2
HALF_COLS = WIN_LON // 2

eps = 1e-05
smear = 0.75
masked = -1e30

LAT = ("x_lo", "z")
LON = ("x_hi", "y", "core")


def normalize(values_in):
    centre = jnp.mean(values_in, -1, keepdims=True)
    offset = values_in - centre
    inverse = lax.rsqrt(jnp.mean(offset * offset, -1, keepdims=True) + eps)
    return (offset * inverse, inverse)


def norm_back(scaled, inverse, upstream):
    return inverse * (
        upstream
        - jnp.mean(upstream, -1, keepdims=True)
        - scaled * jnp.mean(upstream * scaled, -1, keepdims=True)
    )


def gelu_parts(pre_act):
    normal_cdf = 0.5 * (1.0 + lax.erf(pre_act * (1.0 / math.sqrt(2.0))))
    density = jnp.exp(-0.5 * pre_act * pre_act) * (1.0 / math.sqrt(2.0 * math.pi))
    return (pre_act * normal_cdf, normal_cdf + pre_act * density)


def window_row(r, c):
    return ((r // WIN_LAT) * (NCOLS // WIN_LON) + c) * TOK + r % WIN_LAT * WIN_LON


def low_lanes():
    lane = lax.broadcasted_iota(jnp.int32, (1, 2 * HEAD_DIM), 1)
    return (lane < HEAD_DIM).astype(jnp.float32)


def own_lanes(stacked, low):
    return jnp.where(low > 0.5, stacked[:TOK], stacked[TOK:])


def both_heads(pair, low):
    wide = pair.astype(jnp.float32)
    return jnp.concatenate([wide * low, wide * (1.0 - low)], 0).astype(jnp.bfloat16)


def dot_nn(a, b):
    return lax.dot_general(a, b, (((1,), (0,)), ((), ())), preferred_element_type=jnp.float32)


def dot_tn(a, b):
    return lax.dot_general(a, b, (((0,), (0,)), ((), ())), preferred_element_type=jnp.float32)


def dot_nt(a, b):
    return lax.dot_general(a, b, (((1,), (1,)), ((), ())), preferred_element_type=jnp.float32)


def forward_kernel(
    at_ref, main_ref, aux_ref, col_ref, row_ref, corner_ref,
    sort_ref, sort_tall_ref, wqkv_ref, wproj_hbm, wfc1_hbm, wfc2_hbm, whead_hbm,
    xw_ref, qkv_ref, probs_ref, dctx_ref, dres_ref, ctx_ref, gown_ref, gother_ref,
    ctx32_ref, n2_ref, act_ref, slope_ref, dpre_ref, n3_ref, dlog_ref, doutb_ref,
    x32_ref, lines_ref, wproj_ref, wfc1_ref, wfc2_ref, whead_ref, fetched,
):
    fetches = [
        pltpu.make_async_copy(source, target, fetched.at[i])
        for i, (source, target) in enumerate(
            (
                (wproj_hbm, wproj_ref),
                (wfc1_hbm, wfc1_ref),
                (wfc2_hbm, wfc2_ref),
                (whead_hbm, whead_ref),
            )
        )
    ]
    for fetch in fetches:
        fetch.start()
    for r in range(NROWS):
        if r < NROWS - HALF_ROWS:
            lines_ref[r, :NCOLS, :D] = main_ref[r + HALF_ROWS].astype(jnp.float32)
            lines_ref[r, :NCOLS, D:] = aux_ref[r + HALF_ROWS].astype(jnp.float32)
            lines_ref[r, NCOLS : NCOLS + HALF_COLS, :] = col_ref[r].astype(jnp.float32)
        else:
            far = r + HALF_ROWS - NROWS
            lines_ref[r, :NCOLS, :] = row_ref[far].astype(jnp.float32)
            lines_ref[r, NCOLS : NCOLS + HALF_COLS, :] = corner_ref[far].astype(jnp.float32)
        for c in range(NCOLS // WIN_LON):
            first = window_row(r, c)
            x32_ref[first : first + WIN_LON, :] = lines_ref[
                r, c * WIN_LON + HALF_COLS : (c + 1) * WIN_LON + HALF_COLS, :
            ]
    xw_ref[...] = x32_ref[:, :D].astype(jnp.bfloat16)

    def project(c, carry):
        rows = pl.ds(pl.multiple_of(c * CHUNK, CHUNK), CHUNK)
        scaled, _ = normalize(x32_ref[rows, :D])
        normed = scaled.astype(jnp.bfloat16)
        for j in range(3):
            part = dot_nn(normed, wqkv_ref[:, j * D : (j + 1) * D])
            for i in range(CHUNK // TOK):
                qkv_ref[c * (CHUNK // TOK) + i, :, j * D : (j + 1) * D] = part[
                    i * TOK : (i + 1) * TOK
                ].astype(jnp.bfloat16)
        return carry

    lax.fori_loop(0, ROWS // CHUNK, project, 0)

    low = low_lanes()
    q_late = lax.broadcasted_iota(jnp.int32, (2 * TOK, TOK), 0) % TOK >= TOK // 2
    k_late = lax.broadcasted_iota(jnp.int32, (2 * TOK, TOK), 1) >= TOK // 2
    apart = jnp.where(q_late == k_late, 0.0, 1.0)
    last = at_ref[3]

    def attend(w, carry):
        split = jnp.where(jnp.logical_and(last > 0, w >= WINDOWS // 2), 1.0, 0.0)
        block = apart * split
        for pair in range(HEADS // 2):
            at = pair * 2 * HEAD_DIM
            q = both_heads(qkv_ref[w, :, at : at + 128], low)
            k = qkv_ref[w, :, D + at : D + at + 128]
            v = qkv_ref[w, :, 2 * D + at : 2 * D + at + 128]
            s = dot_nt(q, k) * HEAD_DIM ** (-0.5)
            s = jnp.where(block > 0.5, masked, s)
            ex = jnp.exp(s - jnp.max(s, -1, keepdims=True))
            p = (ex / jnp.sum(ex, -1, keepdims=True)).astype(jnp.bfloat16)
            probs_ref[w, pair] = p
            ctx32_ref[pl.ds(pl.multiple_of(w * TOK, 8), TOK), at : at + 128] = own_lanes(
                dot_nn(p, v), low
            )
        return carry

    lax.fori_loop(0, WINDOWS, attend, 0)

    for fetch in fetches:
        fetch.wait()
    edge = lax.broadcasted_iota(jnp.int32, (1, BINS), 1).astype(jnp.float32)
    width = 1.0 / (smear * math.sqrt(2.0))

    def dense(c, carry):
        rows = pl.ds(pl.multiple_of(c * CHUNK, CHUNK), CHUNK)
        ctx = ctx32_ref[rows, :].astype(jnp.bfloat16)
        ctx_ref[rows, :] = dot_nt(ctx, sort_ref[...]).astype(jnp.bfloat16)
        attended = dot_nn(ctx, wproj_ref[...]).astype(jnp.bfloat16)
        residual = x32_ref[rows, :D] + attended.astype(jnp.float32)
        scaled2, inverse2 = normalize(residual)
        n2 = scaled2.astype(jnp.bfloat16)
        n2_ref[rows, :] = dot_nt(n2, sort_ref[...]).astype(jnp.bfloat16)
        out = residual
        for j in range(FF // D):
            cols = slice(j * D, (j + 1) * D)
            act, slope = gelu_parts(dot_nn(n2, wfc1_ref[:, cols]))
            act = act.astype(jnp.bfloat16)
            act_ref[rows, cols] = dot_nt(act, sort_tall_ref[...]).astype(jnp.bfloat16)
            slope_ref[:, cols] = slope
            out = out + dot_nn(act, wfc2_ref[cols, :])
        scaled3, inverse3 = normalize(out)
        n3 = scaled3.astype(jnp.bfloat16)
        n3_ref[rows, :] = dot_nt(n3, sort_ref[...]).astype(jnp.bfloat16)
        extra = x32_ref[rows, D : D + 128]
        weight = extra[:, VARS : VARS + 1] / VARS
        dz = jnp.zeros((CHUNK, D), jnp.float32)
        for v in range(VARS):
            cols = slice(v * BINS, (v + 1) * BINS)
            logits = dot_nn(n3, whead_ref[:, cols])
            ex = jnp.exp(logits - jnp.max(logits, -1, keepdims=True))
            probs = ex / jnp.sum(ex, -1, keepdims=True)
            centre = extra[:, v : v + 1] + 0.5
            mass = lax.erf((edge + 1.0 - centre) * width) - lax.erf((edge - centre) * width)
            total = lax.erf((BINS - centre) * width) - lax.erf((0.0 - centre) * width)
            d_log = (weight * (probs - mass / total)).astype(jnp.bfloat16)
            dlog_ref[rows, cols] = d_log
            dz = dz + dot_nt(d_log, whead_ref[:, cols])
        d_out = norm_back(scaled3, inverse3, dz)
        d_outb = d_out.astype(jnp.bfloat16)
        doutb_ref[rows, :] = d_outb
        dn = jnp.zeros((CHUNK, D), jnp.float32)
        for j in range(FF // D):
            cols = slice(j * D, (j + 1) * D)
            d_pre = (dot_nt(d_outb, wfc2_ref[cols, :]) * slope_ref[:, cols]).astype(jnp.bfloat16)
            dpre_ref[rows, cols] = d_pre
            dn = dn + dot_nt(d_pre, wfc1_ref[:, cols])
        d_res = d_out + norm_back(scaled2, inverse2, dn)
        dres_ref[rows, :] = d_res
        d_ctx = dot_nt(d_res.astype(jnp.bfloat16), wproj_ref[...])
        for i in range(CHUNK // TOK):
            dctx_ref[c * (CHUNK // TOK) + i] = d_ctx[i * TOK : (i + 1) * TOK].astype(jnp.bfloat16)
        return carry

    lax.fori_loop(0, ROWS // CHUNK, dense, 0)

    def keep(at, grad):
        gown_ref[:, at : at + D] = grad[: D // 2].astype(jnp.bfloat16)
        gother_ref[:, at : at + D] = grad[D // 2 :].astype(jnp.bfloat16)

    for j in range(2):
        keep(j * D, dot_tn(n3_ref[...], dlog_ref[:, j * D : (j + 1) * D]))
    for j in range(FF // D):
        cols = slice(j * D, (j + 1) * D)
        keep(2 * D + j * D, dot_tn(n2_ref[...], dpre_ref[:, cols]))
    for m in range(FF // D):
        grad = dot_tn(act_ref[:, m * D : (m + 1) * D], doutb_ref[...]).astype(jnp.bfloat16)
        for t in range(32):
            i1, core, z_low, x_hi = (t // 8, t // 4 % 2, t // 2 % 2, t % 2)
            z = (m % 2 * 2 + z_low + 4 - at_ref[2]) % 4
            x = (x_hi * 2 + m // 2 + 4 - at_ref[0]) % 4
            rows = pl.ds(pl.multiple_of(z * 64 + x * 16, 16), 16)
            target = gother_ref if core else gown_ref
            target[rows, 6 * D + i1 * D : 7 * D + i1 * D] = grad[t * 16 : (t + 1) * 16]


def attention_back_kernel(
    qkv_ref, probs_ref, dctx_ref, dqkv_ref, dqkv32_ref
):
    low = low_lanes()

    def attend(w, carry):
        rows = pl.ds(pl.multiple_of(w * TOK, 8), TOK)
        for pair in range(HEADS // 2):
            at = pair * 2 * HEAD_DIM
            q = both_heads(qkv_ref[w, :, at : at + 128], low)
            k = qkv_ref[w, :, D + at : D + at + 128]
            v = qkv_ref[w, :, 2 * D + at : 2 * D + at + 128]
            up = both_heads(dctx_ref[w, :, at : at + 128], low)
            p = probs_ref[w, pair]
            p32 = p.astype(jnp.float32)
            d_p = dot_nt(up, v)
            d_s = p32 * (d_p - jnp.sum(d_p * p32, -1, keepdims=True)) * HEAD_DIM ** (-0.5)
            d_s = d_s.astype(jnp.bfloat16)
            dqkv32_ref[rows, at : at + 128] = own_lanes(dot_nn(d_s, k), low)
            dqkv32_ref[rows, D + at : D + at + 128] = dot_tn(d_s, q)
            dqkv32_ref[rows, 2 * D + at : 2 * D + at + 128] = dot_tn(p, up)
        return carry

    lax.fori_loop(0, WINDOWS // 2, attend, 0)
    dqkv_ref[...] = dqkv32_ref[...].astype(jnp.bfloat16)


def finish_kernel(
    xw_ref, sort_ref, dqkv_a_ref, dqkv_b_ref, dres_ref, ctx_ref, wqkv_ref,
    glat_ref, gown_ref, gother_ref,
    n1_ref, glat32_ref, line_ref,
):
    half = ROWS // 2
    for c, dqkv_ref in enumerate((dqkv_a_ref, dqkv_b_ref)):
        rows = slice(c * half, (c + 1) * half)
        scaled1, inverse1 = normalize(xw_ref[rows, :].astype(jnp.float32))
        n1_ref[c] = dot_nt(scaled1.astype(jnp.bfloat16), sort_ref[...]).astype(jnp.bfloat16)
        d_sh = dot_nt(dqkv_ref[...], wqkv_ref[...]).astype(jnp.bfloat16).astype(jnp.float32)
        glat32_ref[rows, :] = dres_ref[rows, :] + norm_back(scaled1, inverse1, d_sh)
    for r in range(NROWS):
        for c in range(NCOLS // WIN_LON):
            first = window_row(r, c)
            line_ref[r, c * WIN_LON : (c + 1) * WIN_LON, :] = glat32_ref[
                first : first + WIN_LON, :
            ]
        glat_ref[r] = line_ref[r].astype(jnp.bfloat16)
    for j in range(3):
        cols = slice(j * D, (j + 1) * D)
        grad = dot_tn(n1_ref[0], dqkv_a_ref[:, cols]) + dot_tn(n1_ref[1], dqkv_b_ref[:, cols])
        gown_ref[:, cols] = grad[: D // 2].astype(jnp.bfloat16)
        gother_ref[:, cols] = grad[D // 2 :].astype(jnp.bfloat16)
    grad = dot_tn(ctx_ref[...], dres_ref[...].astype(jnp.bfloat16))
    gown_ref[:, 3 * D :] = grad[: D // 2].astype(jnp.bfloat16)
    gother_ref[:, 3 * D :] = grad[D // 2 :].astype(jnp.bfloat16)


def last_kernel(own_ref, a_ref, b_ref, c_ref, qkv_ref, proj_ref, fc1_ref, fc2_ref, head_ref):
    total = own_ref[...].astype(jnp.float32)
    for ref in (a_ref, b_ref, c_ref):
        total = total + ref[...].astype(jnp.float32)
    qkv_ref[...] = total[:, : 3 * D]
    proj_ref[...] = total[:, 3 * D : 4 * D]
    head_ref[...] = total[:, 4 * D : 6 * D]
    fc1_ref[...] = total[:, 6 * D : 10 * D]
    for i in range(4):
        fc2_ref[4 * i : 4 * i + 4, :] = total[:, (10 + i) * D : (11 + i) * D]


def run_last(own, arrived):
    f32 = jnp.float32
    return pl.pallas_call(
        last_kernel,
        out_shape=(
            whole((4, 3 * D), f32),
            whole((4, D), f32),
            whole((4, FF), f32),
            whole((16, D), f32),
            whole((4, VARS * BINS), f32),
        ),
        in_specs=[VMEM_SPEC] * 4,
        out_specs=(VMEM_SPEC,) * 5,
        compiler_params=pltpu.CompilerParams(vmem_limit_bytes=16 * 1024 * 1024),
        name="last",
    )(own, *arrived)


def whole(shape, dtype):
    return jax.ShapeDtypeStruct(shape, dtype)


VMEM_SPEC = pl.BlockSpec(memory_space=pltpu.VMEM)


def run_forward(at, blocks, sort, sort_tall, w_qkv, w_proj, w_fc1, w_fc2, w_head):
    bf, f32 = (jnp.bfloat16, jnp.float32)
    return pl.pallas_call(
        forward_kernel,
        out_shape=(
            whole((ROWS, D), bf),
            whole((WINDOWS, TOK, 3 * D), bf),
            whole((WINDOWS, HEADS // 2, 2 * TOK, TOK), bf),
            whole((WINDOWS, TOK, D), bf),
            whole((ROWS, D), f32),
            whole((ROWS, D), bf),
            whole((D // 2, 10 * D), bf),
            whole((D // 2, 10 * D), bf),
        ),
        in_specs=[pl.BlockSpec(memory_space=pltpu.SMEM)] + [VMEM_SPEC] * 8
        + [pl.BlockSpec(memory_space=pl.ANY)] * 4,
        out_specs=(VMEM_SPEC,) * 8,
        scratch_shapes=[
            pltpu.VMEM((ROWS, D), f32),
            pltpu.VMEM((ROWS, D), bf),
            pltpu.VMEM((ROWS, FF), bf),
            pltpu.VMEM((CHUNK, FF), f32),
            pltpu.VMEM((ROWS, FF), bf),
            pltpu.VMEM((ROWS, D), bf),
            pltpu.VMEM((ROWS, VARS * BINS), bf),
            pltpu.VMEM((ROWS, D), bf),
            pltpu.VMEM((ROWS, WIDE), f32),
            pltpu.VMEM((NROWS, 80, WIDE), f32),
            pltpu.VMEM((D, D), bf),
            pltpu.VMEM((D, FF), bf),
            pltpu.VMEM((FF, D), bf),
            pltpu.VMEM((D, VARS * BINS), bf),
            pltpu.SemaphoreType.DMA((4,)),
        ],
        compiler_params=pltpu.CompilerParams(vmem_limit_bytes=60 * 1024 * 1024),
        name="forward",
    )(at, *blocks, sort, sort_tall, w_qkv, w_proj, w_fc1, w_fc2, w_head)


def run_attention_back(part, qkv, probs, d_ctx):
    bf, f32 = (jnp.bfloat16, jnp.float32)
    half = WINDOWS // 2
    return pl.pallas_call(
        attention_back_kernel,
        out_shape=whole((ROWS // 2, 3 * D), bf),
        grid=(1,),
        in_specs=[
            pl.BlockSpec((half, TOK, 3 * D), lambda i: (part, 0, 0)),
            pl.BlockSpec((half, HEADS // 2, 2 * TOK, TOK), lambda i: (part, 0, 0, 0)),
            pl.BlockSpec((half, TOK, D), lambda i: (part, 0, 0)),
        ],
        out_specs=pl.BlockSpec((ROWS // 2, 3 * D), lambda i: (0, 0)),
        scratch_shapes=[pltpu.VMEM((ROWS // 2, 3 * D), f32)],
        compiler_params=pltpu.CompilerParams(vmem_limit_bytes=48 * 1024 * 1024),
        name="attention_back",
        cost_estimate=pl.CostEstimate(
            flops=10**9, transcendentals=0, bytes_accessed=4 * 10**6
        ),
    )(qkv, probs, d_ctx)


def run_finish(xw, sort, dqkv_a, dqkv_b, d_res, ctx, w_qkv):
    bf = jnp.bfloat16
    return pl.pallas_call(
        finish_kernel,
        out_shape=(
            whole((NROWS, NCOLS, D), bf),
            whole((D // 2, 4 * D), bf),
            whole((D // 2, 4 * D), bf),
        ),
        in_specs=[VMEM_SPEC] * 7,
        out_specs=(VMEM_SPEC,) * 3,
        scratch_shapes=[
            pltpu.VMEM((2, ROWS // 2, D), bf),
            pltpu.VMEM((ROWS, D), jnp.float32),
            pltpu.VMEM((NROWS, NCOLS, D), jnp.float32),
        ],
        compiler_params=pltpu.CompilerParams(vmem_limit_bytes=48 * 1024 * 1024),
        name="finish",
        cost_estimate=pl.CostEstimate(
            flops=10**9, transcendentals=0, bytes_accessed=8 * 10**6
        ),
    )(xw, sort, dqkv_a, dqkv_b, d_res, ctx, w_qkv)


def place():
    x = lax.axis_index("x_hi") * 2 + lax.axis_index("x_lo")
    return (x, lax.axis_index("y"), lax.axis_index("z"), lax.axis_index("core"))


def sorter():
    x_me, y_me, z_me, core_me = place()
    at = lax.broadcasted_iota(jnp.int32, (D, 1), 0)
    source = lax.broadcasted_iota(jnp.int32, (D, D), 1)
    core = (at // 256 + core_me) % 2
    z = (at // 64 + z_me) % 4
    x = (at // 16 + x_me) % 4
    y = (at // 4 + y_me) % 4
    owner = ((((x % 2) * 4 + z) * 2 + x // 2) * 4 + y) * 2 + core
    return (source == owner * 4 + at % 4).astype(jnp.bfloat16)


def tall_sorter():
    _, y_me, _, core_me = place()
    at = lax.broadcasted_iota(jnp.int32, (D, 1), 0)
    source = lax.broadcasted_iota(jnp.int32, (D, D), 1)
    core = (at // 64 + core_me) % 2
    y = (at // 4 + y_me) % 4
    owner = (at // 16 % 4 * 4 + y) * 2 + core
    return (source == owner * 16 + at // 128 * 4 + at % 4).astype(jnp.bfloat16)


def ring_pairs(axes, step):
    if isinstance(axes, str):
        return [(i, (i + step) % 4) for i in range(4)]
    spot = [(i % 2) * 2 + i // 2 for i in range(4)]
    return [(spot[i], spot[(i + step) % 4]) for i in range(4)]


X = ("x_lo", "x_hi")


def add_up(own, arrived, last=False):
    total = own.astype(jnp.float32)
    for part in arrived:
        total = total + part.astype(jnp.float32)
    return total if last else total.astype(jnp.bfloat16)


def ring_send(blocks, axes):
    return (
        blocks[0],
        [lax.ppermute(blocks[s], axes, ring_pairs(axes, s)) for s in (2, 1, 3)],
    )


def quarters(value):
    n = value.shape[0] // 4
    return [value[i * n : (i + 1) * n] for i in range(4)]


def core_send(value):
    return lax.ppermute(value, "core", [(0, 1), (1, 0)])


def shifted_2(value, axis, steps):
    count = lax.axis_size(axis)
    pairs = [(source, (source + steps) % count) for source in range(count)]
    return lax.ppermute(value, axis, pairs)


def diagonal(value, steps):
    rows, cols = (lax.axis_size(LAT), lax.axis_size(LON))
    pairs = [
        (r * cols + c, (r + steps) % rows * cols + (c + steps) % cols)
        for r in range(rows)
        for c in range(cols)
    ]
    return lax.ppermute(value, LAT + LON, pairs)


def local(latent, w_qkv, w_proj, w_fc1, w_fc2, w_head, target_bins, land_mask):
    bf = jnp.bfloat16

    aux = jnp.concatenate([target_bins, land_mask[:, :, None]], 2).astype(bf)
    aux = lax.optimization_barrier(jnp.pad(aux, ((0, 0), (0, 0), (0, WIDE - D - VARS - 1))))

    def edge(rows, cols):
        return jnp.concatenate([latent[rows, cols], aux[rows, cols]], 2)

    every, top, rest, left = (slice(None), slice(0, 3), slice(3, None), slice(0, 6))
    row_edge = shifted_2(edge(top, every), LAT, -1)
    col_edge = shifted_2(edge(rest, left), LON, -1)
    corner = diagonal(edge(top, left), -1)
    blocks = (latent, aux, col_edge, row_edge, corner)
    last = (lax.axis_index(LAT) == lax.axis_size(LAT) - 1).astype(jnp.int32)
    x_me, y_me, z_me, _ = place()
    at = jnp.stack([x_me, y_me, z_me, last])
    sort = sorter()
    xw, qkv, probs, d_ctx, d_res, ctx, wide_own, wide_other = run_forward(
        at, blocks, sort, tall_sorter(), w_qkv, w_proj, w_fc1, w_fc2, w_head
    )
    wide_got = core_send(wide_other)
    d_qkv_a = run_attention_back(0, qkv, probs, d_ctx)
    wide = ring_send(quarters(add_up(wide_own, [wide_got])), "z")
    d_qkv_b = run_attention_back(1, qkv, probs, d_ctx)
    grad_latent, qkv_own, qkv_other = run_finish(
        xw, sort, d_qkv_a, d_qkv_b, d_res, ctx, w_qkv
    )
    qkv_got = core_send(qkv_other)
    part = add_up(qkv_own, [qkv_got]).reshape(4, 4, 16, 4 * D)
    part = [part[:, s] for s in range(4)]
    part = add_up(*ring_send(part, X))
    wide = add_up(*ring_send(quarters(add_up(*wide)), X))
    part = add_up(*ring_send([part[s] for s in range(4)], "z"))
    both = ring_send(quarters(jnp.concatenate([part, wide], 1)), "y")
    keep_rows, keep_cols = (NROWS - HALF_ROWS, NCOLS - HALF_COLS)
    grad_cols = shifted_2(grad_latent[:keep_rows, keep_cols:], LON, 1)
    grad_rows = shifted_2(grad_latent[keep_rows:, :keep_cols], LAT, 1)
    grad_corner = diagonal(grad_latent[keep_rows:, keep_cols:], 1)
    grad_latent = jnp.concatenate(
        [
            jnp.concatenate([grad_corner, grad_rows], 1),
            jnp.concatenate([grad_cols, grad_latent[:keep_rows, :keep_cols]], 1),
        ],
        0,
    )
    return (grad_latent, *run_last(*both))


def solution(mesh):
    fine = Mesh(mesh.devices.reshape(2, 4, 2, 4, 2), LAT + LON)
    grid = P(LAT, LON)
    rows = P(LAT + LON, None)
    return jax.shard_map(
        local,
        mesh=fine,
        in_specs=(P(LAT, LON, None), P(), P(), P(), P(), P(), P(LAT, LON, None), grid),
        out_specs=(P(LAT, LON, None), rows, rows, rows, rows, rows),
        check_vma=False,
    )
```
